64 devices in a mesh: dp: 4 (over x, y), sp: 16 (over z, core).
Axes of the slice: x: 2, y: 2, z: 8, core: 2. Of those that a mesh axis runs over, the one named last changes fastest.
The devices are a block of a 4x4x8 slice.
Arguments:
- patches: bfloat16 [32768, 1280], P(('dp', 'sp')), parts along dimension 0
- embeds: bfloat16 [16384, 2560], P(('dp', 'sp')), parts along dimension 0
- dest_slot: int32 [8192], P(('dp', 'sp')), parts along dimension 0
- rope_pos: int32 [3, 16384], P(None, ('dp', 'sp')), parts along dimension 1
- cu_doc: int32 [20], P('dp'), parts along dimension 0
- ln_w: bfloat16 [1280], replicated
- ln_b: bfloat16 [1280], replicated
- w_one: bfloat16 [5120, 5120], replicated
- b_one: bfloat16 [5120], replicated
- w_two: bfloat16 [5120, 2560], replicated
- b_two: bfloat16 [2560], replicated
- norm_attn: bfloat16 [2560], replicated
- w_q: bfloat16 [2560, 2560], replicated
- b_q: bfloat16 [2560], replicated
- w_k: bfloat16 [2560, 2560], replicated
- b_k: bfloat16 [2560], replicated
- w_v: bfloat16 [2560, 2560], replicated
- b_v: bfloat16 [2560], replicated
- w_o: bfloat16 [2560, 2560], replicated
- norm_mlp: bfloat16 [2560], replicated
- w_gate: bfloat16 [2560, 6912], replicated
- w_up: bfloat16 [2560, 6912], replicated
- w_down: bfloat16 [6912, 2560], replicated
Outputs:
- output: bfloat16 [16384, 2560], P(('dp', 'sp')), parts along dimension 0
There are 4 independent parts. The reference program is written for one: setup_inputs(seed, part) draws one part's arguments, and reference() takes and returns one part's arrays. A program takes and returns all parts, laid end to end along the dimension named above; an argument that names none is the same for every part.
All inputs are finite; a program needn't handle non-finite values.
Results may differ from the reference program's by a relative error of at most 0.0107878.
Values are sent between devices in bfloat16 or wider.
A program may use at most 768 MiB of HBM per device.

```python
import jax
import jax.numpy as jnp
from jax import lax

GROUP_SIZE = 16
TOK_DEV = 256
MERGED_DEV = 128
HIDDEN = 2560
FFN_DIM = 6912
NUM_HEADS = 20
KV_HEADS = 20
HEAD_DIM = 128
VIT_DIM = 1280
NUM_DOCS = 4

SEQ_LEN = GROUP_SIZE * TOK_DEV
MERGE_DIM = 4 * VIT_DIM
Q_WIDTH = NUM_HEADS * HEAD_DIM
KV_WIDTH = KV_HEADS * HEAD_DIM
NORM_EPS = 1e-6
ROPE_THETA = 1000000.0
MROPE_SPLIT = (16, 40)


def layout_draw(layout_key):
    sub_keys = jax.random.split(layout_key, 7)
    totals = jax.random.randint(sub_keys[0], (GROUP_SIZE,), MERGED_DEV // 4, MERGED_DEV + 1)
    full_dev = jax.random.randint(sub_keys[1], (), 0, GROUP_SIZE)
    totals = jnp.where(jnp.arange(GROUP_SIZE) == full_dev, MERGED_DEV, totals)
    first_len = jax.random.randint(sub_keys[2], (GROUP_SIZE,), 1, totals)
    img_sizes = jnp.stack([first_len, totals - first_len], axis=1).reshape(2 * GROUP_SIZE)
    img_order = jax.random.permutation(sub_keys[3], 2 * GROUP_SIZE)
    text_total = SEQ_LEN - jnp.sum(img_sizes)
    gap_weights = jax.random.randint(sub_keys[4], (2 * GROUP_SIZE + 1,), 1, 17)
    cum_weights = jnp.cumsum(gap_weights)
    text_before = text_total * cum_weights // cum_weights[-1]
    sizes_seq = img_sizes[img_order]
    start_seq = text_before[:-1] + jnp.cumsum(sizes_seq) - sizes_seq
    start_img = jnp.zeros((2 * GROUP_SIZE,), jnp.int32).at[img_order].set(start_seq.astype(jnp.int32))
    row_ids = jnp.arange(GROUP_SIZE * MERGED_DEV)
    dev_of = row_ids // MERGED_DEV
    local_row = row_ids % MERGED_DEV
    first_of = first_len[dev_of]
    second_img = local_row >= first_of
    img_id = 2 * dev_of + second_img.astype(jnp.int32)
    offset = local_row - jnp.where(second_img, first_of, 0)
    dest_slot = jnp.where(local_row < totals[dev_of], start_img[img_id] + offset, -1).astype(jnp.int32)
    doc_cuts = jnp.sort(jax.random.permutation(sub_keys[5], SEQ_LEN - 1)[:NUM_DOCS - 1] + 1).astype(jnp.int32)
    cu_doc = jnp.concatenate([jnp.zeros((1,), jnp.int32), doc_cuts, jnp.full((1,), SEQ_LEN, jnp.int32)])
    tokens = jnp.arange(SEQ_LEN)
    doc_id = jnp.sum(tokens[:, None] >= doc_cuts[None, :], axis=1)
    within = tokens - cu_doc[doc_id]
    is_image = jnp.zeros((SEQ_LEN,), jnp.bool_).at[jnp.where(dest_slot >= 0, dest_slot, SEQ_LEN)].set(True, mode='drop')
    grid_off = jax.random.randint(sub_keys[6], (2, SEQ_LEN), 0, 32)
    rope_pos = jnp.stack([within, within + jnp.where(is_image, grid_off[0], 0), within + jnp.where(is_image, grid_off[1], 0)]).astype(jnp.int32)
    return dest_slot, rope_pos, cu_doc


def gauss_draw(draw_key, shape, scale):
    return jax.random.normal(draw_key, shape, jnp.float32) * scale


def setup_inputs(seed: int = 0, part: int = 0) -> dict:
    root = jax.random.key(seed)
    part_key = jax.random.fold_in(root, part)
    layout_key, patch_key, embed_key = jax.random.split(part_key, 3)
    dest_slot, rope_pos, cu_doc = layout_draw(layout_key)
    wkeys = jax.random.split(jax.random.fold_in(root, 100003), 18)
    bf_type = jnp.bfloat16
    return dict(
        patches=gauss_draw(patch_key, (GROUP_SIZE * 4 * MERGED_DEV, VIT_DIM), 1.0).astype(bf_type),
        embeds=gauss_draw(embed_key, (SEQ_LEN, HIDDEN), 1.0).astype(bf_type),
        dest_slot=dest_slot,
        rope_pos=rope_pos,
        cu_doc=cu_doc,
        ln_w=(1.0 + gauss_draw(wkeys[0], (VIT_DIM,), 0.3)).astype(bf_type),
        ln_b=gauss_draw(wkeys[1], (VIT_DIM,), 0.3).astype(bf_type),
        w_one=gauss_draw(wkeys[2], (MERGE_DIM, MERGE_DIM), MERGE_DIM ** -0.5).astype(bf_type),
        b_one=gauss_draw(wkeys[3], (MERGE_DIM,), 0.5).astype(bf_type),
        w_two=gauss_draw(wkeys[4], (MERGE_DIM, HIDDEN), MERGE_DIM ** -0.5).astype(bf_type),
        b_two=gauss_draw(wkeys[5], (HIDDEN,), 0.5).astype(bf_type),
        norm_attn=(1.0 + gauss_draw(wkeys[6], (HIDDEN,), 0.3)).astype(bf_type),
        w_q=gauss_draw(wkeys[7], (HIDDEN, Q_WIDTH), 1.6 * HIDDEN ** -0.5).astype(bf_type),
        b_q=gauss_draw(wkeys[8], (Q_WIDTH,), 0.5).astype(bf_type),
        w_k=gauss_draw(wkeys[9], (HIDDEN, KV_WIDTH), 1.6 * HIDDEN ** -0.5).astype(bf_type),
        b_k=gauss_draw(wkeys[10], (KV_WIDTH,), 0.5).astype(bf_type),
        w_v=gauss_draw(wkeys[11], (HIDDEN, KV_WIDTH), HIDDEN ** -0.5).astype(bf_type),
        b_v=gauss_draw(wkeys[12], (KV_WIDTH,), 0.5).astype(bf_type),
        w_o=gauss_draw(wkeys[13], (Q_WIDTH, HIDDEN), Q_WIDTH ** -0.5).astype(bf_type),
        norm_mlp=(1.0 + gauss_draw(wkeys[14], (HIDDEN,), 0.3)).astype(bf_type),
        w_gate=gauss_draw(wkeys[15], (HIDDEN, FFN_DIM), HIDDEN ** -0.5).astype(bf_type),
        w_up=gauss_draw(wkeys[16], (HIDDEN, FFN_DIM), HIDDEN ** -0.5).astype(bf_type),
        w_down=gauss_draw(wkeys[17], (FFN_DIM, HIDDEN), FFN_DIM ** -0.5).astype(bf_type),
    )


def layer_norm(values_in, gain_vec, shift_vec):
    widened = values_in.astype(jnp.float32)
    centered = widened - jnp.mean(widened, axis=-1, keepdims=True)
    spread = jnp.mean(centered * centered, axis=-1, keepdims=True)
    return (centered * lax.rsqrt(spread + NORM_EPS) * gain_vec.astype(jnp.float32) + shift_vec.astype(jnp.float32)).astype(jnp.bfloat16)


def rms_norm(values_in, gain_vec):
    widened = values_in.astype(jnp.float32)
    return (widened * lax.rsqrt(jnp.mean(widened * widened, axis=-1, keepdims=True) + NORM_EPS) * gain_vec.astype(jnp.float32)).astype(jnp.bfloat16)


def merger_mlp(grouped, w_one, b_one, w_two, b_two):
    inner = jax.nn.gelu(jnp.dot(grouped, w_one, preferred_element_type=jnp.float32) + b_one.astype(jnp.float32), approximate=False).astype(jnp.bfloat16)
    return (jnp.dot(inner, w_two, preferred_element_type=jnp.float32) + b_two.astype(jnp.float32)).astype(jnp.bfloat16)


def rope_tables(rope_pos):
    inv_freq = ROPE_THETA ** (-jnp.arange(0, HEAD_DIM, 2, dtype=jnp.float32) / HEAD_DIM)
    freq_idx = jnp.arange(HEAD_DIM // 2)[None, :]
    chosen = jnp.where(freq_idx < MROPE_SPLIT[0], rope_pos[0][:, None], jnp.where(freq_idx < MROPE_SPLIT[1], rope_pos[1][:, None], rope_pos[2][:, None]))
    angles = chosen.astype(jnp.float32) * inv_freq[None, :]
    angles = jnp.concatenate([angles, angles], axis=-1)
    return jnp.cos(angles), jnp.sin(angles)


def apply_rope(heads_in, cos_t, sin_t):
    half_dim = HEAD_DIM // 2
    rotated = jnp.concatenate([-heads_in[..., half_dim:], heads_in[..., :half_dim]], axis=-1)
    return heads_in * cos_t[:, None, :] + rotated * sin_t[:, None, :]


def reference(patches, embeds, dest_slot, rope_pos, cu_doc, ln_w, ln_b, w_one, b_one, w_two, b_two, norm_attn, w_q, b_q, w_k, b_k, w_v, b_v, w_o, norm_mlp, w_gate, w_up, w_down):
    normed = layer_norm(patches, ln_w, ln_b).reshape(GROUP_SIZE * MERGED_DEV, MERGE_DIM)
    merged = merger_mlp(normed, w_one, b_one, w_two, b_two)
    target = jnp.where(dest_slot >= 0, dest_slot, SEQ_LEN)
    h_zero = embeds.at[target].set(merged, mode='drop')
    normed_a = rms_norm(h_zero, norm_attn)
    cos_t, sin_t = rope_tables(rope_pos)
    q_lin = jnp.dot(normed_a, w_q, preferred_element_type=jnp.float32) + b_q.astype(jnp.float32)
    k_lin = jnp.dot(normed_a, w_k, preferred_element_type=jnp.float32) + b_k.astype(jnp.float32)
    queries = apply_rope(q_lin.reshape(SEQ_LEN, NUM_HEADS, HEAD_DIM), cos_t, sin_t).astype(jnp.bfloat16)
    keys_rot = apply_rope(k_lin.reshape(SEQ_LEN, KV_HEADS, HEAD_DIM), cos_t, sin_t).astype(jnp.bfloat16)
    values_bf = (jnp.dot(normed_a, w_v, preferred_element_type=jnp.float32) + b_v.astype(jnp.float32)).astype(jnp.bfloat16).reshape(SEQ_LEN, KV_HEADS, HEAD_DIM)
    key_pos = jnp.arange(SEQ_LEN)
    doc_id = jnp.sum(key_pos[:, None] >= cu_doc[None, 1:NUM_DOCS], axis=1)
    keys_wide = keys_rot.astype(jnp.float32)
    values_wide = values_bf.astype(jnp.float32)
    q_blocks = queries.reshape(GROUP_SIZE, TOK_DEV, KV_HEADS, NUM_HEADS // KV_HEADS, HEAD_DIM)

    def attend(block_args):
        block_idx, q_block = block_args
        query_pos = block_idx * TOK_DEV + jnp.arange(TOK_DEV)
        query_doc = lax.dynamic_slice(doc_id, (block_idx * TOK_DEV,), (TOK_DEV,))
        allowed = (key_pos[None, :] <= query_pos[:, None]) & (query_doc[:, None] == doc_id[None, :])
        scores = jnp.einsum('qkgd,tkd->kgqt', q_block.astype(jnp.float32), keys_wide) * HEAD_DIM ** -0.5
        probs_bf = jax.nn.softmax(jnp.where(allowed, scores, -1e30), axis=-1).astype(jnp.bfloat16)
        return jnp.einsum('kgqt,tkd->qkgd', probs_bf.astype(jnp.float32), values_wide).astype(jnp.bfloat16)

    attn_out = lax.map(attend, (jnp.arange(GROUP_SIZE), q_blocks)).reshape(SEQ_LEN, Q_WIDTH)
    h_one = (h_zero.astype(jnp.float32) + jnp.dot(attn_out, w_o, preferred_element_type=jnp.float32)).astype(jnp.bfloat16)
    normed_m = rms_norm(h_one, norm_mlp)
    gate_pre = jnp.dot(normed_m, w_gate, preferred_element_type=jnp.float32)
    up_pre = jnp.dot(normed_m, w_up, preferred_element_type=jnp.float32)
    activated = (jax.nn.silu(gate_pre) * up_pre).astype(jnp.bfloat16)
    return (h_one.astype(jnp.float32) + jnp.dot(activated, w_down, preferred_element_type=jnp.float32)).astype(jnp.bfloat16)
```

```python
import functools

import jax
import jax.numpy as jnp
from jax import lax
from jax.experimental import pallas as pl
from jax.experimental.pallas import tpu as pltpu
from jax.sharding import PartitionSpec as P

HEAD_DIM = 128
NORM_EPS = 1e-6
ROPE_THETA = 1000000.0
MROPE_SPLIT = (16, 40)
MESH = pl.DeviceIdType.MESH
VMEM_LIMIT = 60 * 1024 * 1024


def layer_norm(values_in, gain_vec, shift_vec):
    widened = values_in.astype(jnp.float32)
    centered = widened - jnp.mean(widened, axis=-1, keepdims=True)
    spread = jnp.mean(centered * centered, axis=-1, keepdims=True)
    return (centered * lax.rsqrt(spread + NORM_EPS) * gain_vec.astype(jnp.float32) + shift_vec.astype(jnp.float32)).astype(jnp.bfloat16)


def rms_norm(values_in, gain_vec):
    widened = values_in.astype(jnp.float32)
    return (widened * lax.rsqrt(jnp.mean(widened * widened, axis=-1, keepdims=True) + NORM_EPS) * gain_vec.astype(jnp.float32)).astype(jnp.bfloat16)


def merger_mlp(grouped, w_one, b_one, w_two, b_two):
    inner = jax.nn.gelu(jnp.dot(grouped, w_one, preferred_element_type=jnp.float32) + b_one.astype(jnp.float32), approximate=False).astype(jnp.bfloat16)
    return (jnp.dot(inner, w_two, preferred_element_type=jnp.float32) + b_two.astype(jnp.float32)).astype(jnp.bfloat16)


def rope_tables(rope_pos):
    inv_freq = ROPE_THETA ** (-jnp.arange(0, HEAD_DIM, 2, dtype=jnp.float32) / HEAD_DIM)
    freq_idx = jnp.arange(HEAD_DIM // 2)[None, :]
    chosen = jnp.where(freq_idx < MROPE_SPLIT[0], rope_pos[0][:, None], jnp.where(freq_idx < MROPE_SPLIT[1], rope_pos[1][:, None], rope_pos[2][:, None]))
    angles = chosen.astype(jnp.float32) * inv_freq[None, :]
    cos_h, sin_h = jnp.cos(angles), jnp.sin(angles)
    return jnp.concatenate([cos_h, cos_h], axis=-1), jnp.concatenate([-sin_h, sin_h], axis=-1)


def first_head(dev, group, heads):
    return (dev * heads + group - 1) // group


def owner_of(head, group, heads):
    return head * group // heads


def greet_group(group, me):
    barrier = pltpu.get_barrier_semaphore()
    for k in range(1, group):
        pl.semaphore_signal(barrier, inc=1, device_id={"sp": lax.rem(me + k, group)}, device_id_type=MESH)
    pl.semaphore_wait(barrier, group - 1)


def qkv_send_kernel(group, heads, a_ref, cos_ref, sin_ref, bias_ref, wq_ref, wk_ref, wv_ref, out_ref, wbuf, stage, w_sem, send_sem, recv_sem, own_sem):
    me = lax.axis_index("sp")
    depth = wbuf.shape[0]
    half = heads // 2
    mine = first_head(me, group, heads)

    def head_at(p):
        step = p // 2
        delta = step - (p % 2) * (2 * step + 1)
        return (mine + half + delta + heads) % heads

    def weight_copies(p):
        cols = pl.ds(pl.multiple_of(head_at(p) * HEAD_DIM, HEAD_DIM), HEAD_DIM)
        slot = p % depth
        return [
            pltpu.make_async_copy(w.at[:, cols], wbuf.at[slot, :, pl.ds(n * HEAD_DIM, HEAD_DIM)], w_sem.at[slot, n])
            for n, w in enumerate((wq_ref, wk_ref, wv_ref))
        ]

    def remote(p):
        head = head_at(p)
        target = owner_of(head, group, heads)
        slot = head - first_head(target, group, heads)
        copy = pltpu.make_async_remote_copy(
            src_ref=stage.at[p],
            dst_ref=out_ref.at[slot, :, me],
            send_sem=send_sem.at[p],
            recv_sem=recv_sem.at[slot],
            device_id={"sp": target},
            device_id_type=MESH,
        )
        local = pltpu.make_async_copy(stage.at[p], out_ref.at[slot, :, me], own_sem.at[slot])
        return target, copy, local

    def send(p):
        target, copy, local = remote(p)

        @pl.when(target != me)
        def _():
            copy.start()

        @pl.when(target == me)
        def _():
            local.start()

    for p in range(depth - 1):
        for c in weight_copies(p):
            c.start()
    greet_group(group, me)

    def step(p, carry):
        @pl.when(p + depth - 1 < heads)
        def _():
            for c in weight_copies(p + depth - 1):
                c.start()

        for c in weight_copies(p):
            c.wait()
        lin = jnp.dot(a_ref[...], wbuf[p % depth], preferred_element_type=jnp.float32) + bias_ref[head_at(p)]

        @pl.when(p > 0)
        def _():
            send(p - 1)

        cos_t, sin_t = cos_ref[...], sin_ref[...]
        for n in range(3):
            part = lin[:, n * HEAD_DIM:(n + 1) * HEAD_DIM]
            if n < 2:
                part = part * cos_t + pltpu.roll(part, HEAD_DIM // 2, 1) * sin_t
            stage[p, n] = part.astype(jnp.bfloat16)
        return carry

    lax.fori_loop(0, heads, step, 0)
    send(heads - 1)

    def drain(p, carry):
        target, copy, local = remote(p)

        @pl.when(target != me)
        def _():
            copy.wait_send()

        @pl.when(target == me)
        def _():
            local.wait()

        return carry

    lax.fori_loop(0, heads, drain, 0)
    count = first_head(me + 1, group, heads) - mine
    for slot in range(out_ref.shape[0]):
        landed = out_ref.at[slot, :, pl.ds(0, group - 1)]

        @pl.when(slot < count)
        def _():
            pltpu.make_async_copy(landed, landed, recv_sem.at[slot]).wait()


def qkv_send(group, heads, normed, cos_t, sin_t, biases, w_q, w_k, w_v):
    tokens, width = normed.shape
    slots = -(-heads // group)
    vmem = pl.BlockSpec(memory_space=pltpu.VMEM)
    hbm = pl.BlockSpec(memory_space=pl.ANY)
    return pl.pallas_call(
        functools.partial(qkv_send_kernel, group, heads),
        out_shape=jax.ShapeDtypeStruct((slots, 3, group, tokens, HEAD_DIM), jnp.bfloat16),
        in_specs=[vmem, vmem, vmem, vmem, hbm, hbm, hbm],
        out_specs=hbm,
        scratch_shapes=[
            pltpu.VMEM((3, width, 3 * HEAD_DIM), jnp.bfloat16),
            pltpu.VMEM((heads, 3, tokens, HEAD_DIM), jnp.bfloat16),
            pltpu.SemaphoreType.DMA((3, 3)),
            pltpu.SemaphoreType.DMA((heads,)),
            pltpu.SemaphoreType.DMA((slots,)),
            pltpu.SemaphoreType.DMA((slots,)),
        ],
        compiler_params=pltpu.CompilerParams(collective_id=0, has_side_effects=True, vmem_limit_bytes=VMEM_LIMIT),
        cost_estimate=pl.CostEstimate(flops=2 * tokens * width * 3 * heads * HEAD_DIM, bytes_accessed=3 * width * heads * HEAD_DIM * 2, transcendentals=0),
        name="qkv_send",
    )(normed, cos_t, sin_t, biases, w_q, w_k, w_v)


def attention_kernel(q_rows, k_rows, cuts, info_ref, q_ref, k_ref, v_ref, o_ref):
    slot, block = pl.program_id(0), pl.program_id(1)

    @pl.when(slot < info_ref[0])
    def _():
        start = block * q_rows
        low = 0
        for d in range(cuts):
            low = jnp.where(start >= info_ref[1 + d], info_ref[1 + d], low)
        q_pos = start + lax.broadcasted_iota(jnp.int32, (q_rows, 1), 0)
        q_low = jnp.zeros((q_rows, 1), jnp.int32)
        for d in range(cuts):
            q_low = jnp.where(q_pos >= info_ref[1 + d], info_ref[1 + d], q_low)
        q_val = q_ref[...]
        scale = HEAD_DIM ** -0.5

        def step(j, carry):
            top, total, acc = carry
            rows = pl.ds(pl.multiple_of(j * k_rows, k_rows), k_rows)
            scores = lax.dot_general(q_val, k_ref[rows, :], (((1,), (1,)), ((), ())), preferred_element_type=jnp.float32) * scale
            k_pos = j * k_rows + lax.broadcasted_iota(jnp.int32, (1, k_rows), 1)
            scores = jnp.where((k_pos <= q_pos) & (k_pos >= q_low), scores, -1e30)
            new_top = jnp.maximum(top, jnp.max(scores, axis=1, keepdims=True))
            decay = jnp.exp(top - new_top)
            probs = jnp.exp(scores - new_top)
            total = total * decay + jnp.sum(probs, axis=1, keepdims=True)
            acc = acc * decay + jnp.dot(probs.astype(jnp.bfloat16), v_ref[rows, :], preferred_element_type=jnp.float32)
            return new_top, total, acc

        init = (
            jnp.full((q_rows, 1), -1e30, jnp.float32),
            jnp.zeros((q_rows, 1), jnp.float32),
            jnp.zeros((q_rows, HEAD_DIM), jnp.float32),
        )
        last = (start + q_rows - 1) // k_rows
        _, total, acc = lax.fori_loop(last - (last - low // k_rows), last + 1, step, init)
        o_ref[...] = (acc / total).astype(jnp.bfloat16)


def attention(info, qkv, cuts, q_rows, k_rows):
    slots, _, group, tokens, _ = qkv.shape
    seq = group * tokens
    flat = qkv.reshape(slots, 3, seq, HEAD_DIM)
    blocks = seq // q_rows

    def whole(part):
        return pl.BlockSpec((None, None, seq, HEAD_DIM), lambda s, i, info: (s, part, 0, 0))

    return pl.pallas_call(
        functools.partial(attention_kernel, q_rows, k_rows, cuts),
        grid_spec=pltpu.PrefetchScalarGridSpec(
            num_scalar_prefetch=1,
            grid=(slots, blocks),
            in_specs=[pl.BlockSpec((None, None, q_rows, HEAD_DIM), lambda s, i, info: (s, 0, i, 0)), whole(1), whole(2)],
            out_specs=pl.BlockSpec((None, q_rows, HEAD_DIM), lambda s, i, info: (s, i, 0)),
        ),
        out_shape=jax.ShapeDtypeStruct((slots, seq, HEAD_DIM), jnp.bfloat16),
        compiler_params=pltpu.CompilerParams(vmem_limit_bytes=VMEM_LIMIT),
        cost_estimate=pl.CostEstimate(flops=4 * seq * seq * HEAD_DIM, bytes_accessed=8 * seq * HEAD_DIM * slots, transcendentals=seq * seq // 2),
        name="attention",
    )(info, flat, flat, flat).reshape(slots, group, tokens, HEAD_DIM)


def out_send_kernel(group, heads, o_ref, attn_ref, send_sem, recv_sem, own_sem):
    me = lax.axis_index("sp")
    mine = first_head(me, group, heads)
    count = first_head(me + 1, group, heads) - mine
    slots = o_ref.shape[0]
    greet_group(group, me)

    def hop(k):
        step = k // 2
        return (me + group // 2 + step - (k % 2) * (2 * step + 1) + group) % group

    def out_copy(slot, k):
        head = mine + slot
        cols = pl.ds(pl.multiple_of(head * HEAD_DIM, HEAD_DIM), HEAD_DIM)
        return pltpu.make_async_remote_copy(
            src_ref=o_ref.at[slot, hop(k)],
            dst_ref=attn_ref.at[:, cols],
            send_sem=send_sem.at[slot, k],
            recv_sem=recv_sem.at[head],
            device_id={"sp": hop(k)},
            device_id_type=MESH,
        )

    def own_copy(slot):
        cols = pl.ds(pl.multiple_of((mine + slot) * HEAD_DIM, HEAD_DIM), HEAD_DIM)
        return pltpu.make_async_copy(o_ref.at[slot, me], attn_ref.at[:, cols], own_sem.at[slot])

    for slot in range(slots):

        @pl.when(slot < count)
        def _():
            for k in range(group - 1):
                out_copy(slot, k).start()
            own_copy(slot).start()

    for slot in range(slots):

        @pl.when(slot < count)
        def _():
            for k in range(group - 1):
                out_copy(slot, k).wait_send()
            own_copy(slot).wait()

    def landed(head, carry):
        @pl.when(owner_of(head, group, heads) != me)
        def _():
            block = attn_ref.at[:, pl.ds(pl.multiple_of(head * HEAD_DIM, HEAD_DIM), HEAD_DIM)]
            pltpu.make_async_copy(block, block, recv_sem.at[head]).wait()

        return carry

    lax.fori_loop(0, heads, landed, 0)


def out_send(group, heads, o_heads):
    slots, _, tokens, _ = o_heads.shape
    hbm = pl.BlockSpec(memory_space=pl.ANY)
    return pl.pallas_call(
        functools.partial(out_send_kernel, group, heads),
        out_shape=jax.ShapeDtypeStruct((tokens, heads * HEAD_DIM), jnp.bfloat16),
        in_specs=[hbm],
        out_specs=hbm,
        scratch_shapes=[
            pltpu.SemaphoreType.DMA((slots, group - 1)),
            pltpu.SemaphoreType.DMA((heads,)),
            pltpu.SemaphoreType.DMA((slots,)),
        ],
        compiler_params=pltpu.CompilerParams(collective_id=1, has_side_effects=True),
        name="out_send",
    )(o_heads)


def mlp_residual(h_one, norm_mlp, w_gate, w_up, w_down):
    normed_m = rms_norm(h_one, norm_mlp)
    gate_pre = jnp.dot(normed_m, w_gate, preferred_element_type=jnp.float32)
    up_pre = jnp.dot(normed_m, w_up, preferred_element_type=jnp.float32)
    activated = (jax.nn.silu(gate_pre) * up_pre).astype(jnp.bfloat16)
    return (h_one.astype(jnp.float32) + jnp.dot(activated, w_down, preferred_element_type=jnp.float32)).astype(jnp.bfloat16)


def solution(mesh):
    group = mesh.shape['sp']
    row_spec = P(('dp', 'sp'), None)

    def local_step(patches, embeds, dest_slot, rope_pos, cu_doc, ln_w, ln_b, w_one, b_one, w_two, b_two, norm_attn, w_q, b_q, w_k, b_k, w_v, b_v, w_o, norm_mlp, w_gate, w_up, w_down):
        tok_dev = embeds.shape[0]
        merged_dev = dest_slot.shape[0]
        heads = w_q.shape[1] // HEAD_DIM
        me = lax.axis_index('sp')
        all_slots = lax.all_gather(dest_slot, 'sp', tiled=True)
        normed = layer_norm(patches, ln_w, ln_b).reshape(merged_dev, -1)
        merged = merger_mlp(normed, w_one, b_one, w_two, b_two)
        all_merged = lax.all_gather(merged, 'sp', tiled=True)
        pick = all_slots[None, :] == (me * tok_dev + jnp.arange(tok_dev))[:, None]
        placed = jnp.dot(pick.astype(jnp.bfloat16), all_merged, preferred_element_type=jnp.float32).astype(jnp.bfloat16)
        h_zero = jnp.where(jnp.any(pick, axis=1)[:, None], placed, embeds)
        cos_t, sin_t = rope_tables(rope_pos)
        biases = jnp.concatenate([b.astype(jnp.float32).reshape(heads, 1, HEAD_DIM) for b in (b_q, b_k, b_v)], axis=2)
        qkv = qkv_send(group, heads, rms_norm(h_zero, norm_attn), cos_t, sin_t, biases, w_q, w_k, w_v)
        count = first_head(me + 1, group, heads) - first_head(me, group, heads)
        cuts = cu_doc.shape[0] - 2
        info = jnp.concatenate([count.astype(jnp.int32).reshape(1), cu_doc[1:-1]])
        o_heads = attention(info, qkv, cuts, 256, 256)
        attn_out = out_send(group, heads, o_heads)
        h_one = (h_zero.astype(jnp.float32) + jnp.dot(attn_out, w_o, preferred_element_type=jnp.float32)).astype(jnp.bfloat16)
        return mlp_residual(h_one, norm_mlp, w_gate, w_up, w_down)

    in_specs = (row_spec, row_spec, P(('dp', 'sp')), P(None, ('dp', 'sp')), P('dp')) + (P(),) * 18
    return jax.shard_map(local_step, mesh=mesh, in_specs=in_specs, out_specs=row_spec, check_vma=False)
```

```python
import functools

import jax
import jax.numpy as jnp
from jax import lax
from jax.experimental import pallas as pl
from jax.experimental.pallas import tpu as pltpu
from jax.sharding import PartitionSpec as P

HEAD_DIM = 128
NORM_EPS = 1e-6
ROPE_THETA = 1000000.0
MROPE_SPLIT = (16, 40)
MESH = pl.DeviceIdType.MESH
VMEM_LIMIT = 60 * 1024 * 1024


def layer_norm(values_in, gain_vec, shift_vec):
    widened = values_in.astype(jnp.float32)
    centered = widened - jnp.mean(widened, axis=-1, keepdims=True)
    spread = jnp.mean(centered * centered, axis=-1, keepdims=True)
    return (centered * lax.rsqrt(spread + NORM_EPS) * gain_vec.astype(jnp.float32) + shift_vec.astype(jnp.float32)).astype(jnp.bfloat16)


def rms_norm(values_in, gain_vec):
    widened = values_in.astype(jnp.float32)
    return (widened * lax.rsqrt(jnp.mean(widened * widened, axis=-1, keepdims=True) + NORM_EPS) * gain_vec.astype(jnp.float32)).astype(jnp.bfloat16)


def merger_mlp(grouped, w_one, b_one, w_two, b_two):
    inner = jax.nn.gelu(jnp.dot(grouped, w_one, preferred_element_type=jnp.float32) + b_one.astype(jnp.float32), approximate=False).astype(jnp.bfloat16)
    return (jnp.dot(inner, w_two, preferred_element_type=jnp.float32) + b_two.astype(jnp.float32)).astype(jnp.bfloat16)


def rope_tables(rope_pos):
    inv_freq = ROPE_THETA ** (-jnp.arange(0, HEAD_DIM, 2, dtype=jnp.float32) / HEAD_DIM)
    freq_idx = jnp.arange(HEAD_DIM // 2)[None, :]
    chosen = jnp.where(freq_idx < MROPE_SPLIT[0], rope_pos[0][:, None], jnp.where(freq_idx < MROPE_SPLIT[1], rope_pos[1][:, None], rope_pos[2][:, None]))
    angles = chosen.astype(jnp.float32) * inv_freq[None, :]
    cos_h, sin_h = jnp.cos(angles), jnp.sin(angles)
    return jnp.concatenate([cos_h, cos_h], axis=-1), jnp.concatenate([-sin_h, sin_h], axis=-1)


def first_head(dev, group, heads):
    return (dev * heads + group - 1) // group


def owner_of(head, group, heads):
    return head * group // heads


def greet_group(group, me):
    barrier = pltpu.get_barrier_semaphore()
    for k in range(1, group):
        pl.semaphore_signal(barrier, inc=1, device_id={"sp": lax.rem(me + k, group)}, device_id_type=MESH)
    pl.semaphore_wait(barrier, group - 1)


def qkv_send_kernel(group, heads, a_ref, cos_ref, sin_ref, bias_ref, wq_ref, wk_ref, wv_ref, out_ref, wbuf, stage, w_sem, send_sem, recv_sem, own_sem):
    me = lax.axis_index("sp")
    depth = wbuf.shape[0]
    half = heads // 2
    mine = first_head(me, group, heads)

    def head_at(p):
        step = p // 2
        delta = step - (p % 2) * (2 * step + 1)
        return (mine + half + delta + heads) % heads

    def weight_copies(p):
        cols = pl.ds(pl.multiple_of(head_at(p) * HEAD_DIM, HEAD_DIM), HEAD_DIM)
        slot = p % depth
        return [
            pltpu.make_async_copy(w.at[:, cols], wbuf.at[slot, :, pl.ds(n * HEAD_DIM, HEAD_DIM)], w_sem.at[slot, n])
            for n, w in enumerate((wq_ref, wk_ref, wv_ref))
        ]

    def remote(p):
        head = head_at(p)
        target = owner_of(head, group, heads)
        slot = head - first_head(target, group, heads)
        copy = pltpu.make_async_remote_copy(
            src_ref=stage.at[p],
            dst_ref=out_ref.at[slot, :, me],
            send_sem=send_sem.at[p],
            recv_sem=recv_sem.at[slot],
            device_id={"sp": target},
            device_id_type=MESH,
        )
        local = pltpu.make_async_copy(stage.at[p], out_ref.at[slot, :, me], own_sem.at[slot])
        return target, copy, local

    def send(p):
        target, copy, local = remote(p)

        @pl.when(target != me)
        def _():
            copy.start()

        @pl.when(target == me)
        def _():
            local.start()

    for p in range(depth - 1):
        for c in weight_copies(p):
            c.start()
    greet_group(group, me)

    def step(p, carry):
        @pl.when(p + depth - 1 < heads)
        def _():
            for c in weight_copies(p + depth - 1):
                c.start()

        for c in weight_copies(p):
            c.wait()
        lin = jnp.dot(a_ref[...], wbuf[p % depth], preferred_element_type=jnp.float32) + bias_ref[head_at(p)]

        @pl.when(p > 0)
        def _():
            send(p - 1)

        cos_t, sin_t = cos_ref[...], sin_ref[...]
        for n in range(3):
            part = lin[:, n * HEAD_DIM:(n + 1) * HEAD_DIM]
            if n < 2:
                part = part * cos_t + pltpu.roll(part, HEAD_DIM // 2, 1) * sin_t
            stage[p, n] = part.astype(jnp.bfloat16)
        return carry

    lax.fori_loop(0, heads, step, 0)
    send(heads - 1)

    def drain(p, carry):
        target, copy, local = remote(p)

        @pl.when(target != me)
        def _():
            copy.wait_send()

        @pl.when(target == me)
        def _():
            local.wait()

        return carry

    lax.fori_loop(0, heads, drain, 0)
    count = first_head(me + 1, group, heads) - mine
    for slot in range(out_ref.shape[0]):
        landed = out_ref.at[slot, :, pl.ds(0, group - 1)]

        @pl.when(slot < count)
        def _():
            pltpu.make_async_copy(landed, landed, recv_sem.at[slot]).wait()


def qkv_send(group, heads, normed, cos_t, sin_t, biases, w_q, w_k, w_v):
    tokens, width = normed.shape
    slots = -(-heads // group)
    vmem = pl.BlockSpec(memory_space=pltpu.VMEM)
    hbm = pl.BlockSpec(memory_space=pl.ANY)
    return pl.pallas_call(
        functools.partial(qkv_send_kernel, group, heads),
        out_shape=jax.ShapeDtypeStruct((slots, 3, group, tokens, HEAD_DIM), jnp.bfloat16),
        in_specs=[vmem, vmem, vmem, vmem, hbm, hbm, hbm],
        out_specs=hbm,
        scratch_shapes=[
            pltpu.VMEM((3, width, 3 * HEAD_DIM), jnp.bfloat16),
            pltpu.VMEM((heads, 3, tokens, HEAD_DIM), jnp.bfloat16),
            pltpu.SemaphoreType.DMA((3, 3)),
            pltpu.SemaphoreType.DMA((heads,)),
            pltpu.SemaphoreType.DMA((slots,)),
            pltpu.SemaphoreType.DMA((slots,)),
        ],
        compiler_params=pltpu.CompilerParams(collective_id=0, has_side_effects=True, vmem_limit_bytes=VMEM_LIMIT),
        cost_estimate=pl.CostEstimate(flops=2 * tokens * width * 3 * heads * HEAD_DIM, bytes_accessed=3 * width * heads * HEAD_DIM * 2, transcendentals=0),
        name="qkv_send",
    )(normed, cos_t, sin_t, biases, w_q, w_k, w_v)


def attention_kernel(q_rows, k_rows, cuts, info_ref, q_ref, k_ref, v_ref, o_ref):
    slots = q_ref.shape[0]
    start = pl.program_id(0) * q_rows
    low, high = 0, 0
    for d in range(cuts):
        low = jnp.where(start >= info_ref[1 + d], info_ref[1 + d], low)
        high = jnp.where(start + q_rows - 1 >= info_ref[1 + d], info_ref[1 + d], high)
    q_pos = start + lax.broadcasted_iota(jnp.int32, (q_rows, 1), 0)
    q_low = jnp.zeros((q_rows, 1), jnp.int32)
    for d in range(cuts):
        q_low = jnp.where(q_pos >= info_ref[1 + d], info_ref[1 + d], q_low)
    scale = HEAD_DIM ** -0.5 * 1.4426950408889634
    first = low // k_rows
    diag = start // k_rows
    inner = jnp.minimum((high + k_rows - 1) // k_rows, diag)
    last = (start + q_rows - 1) // k_rows

    def run(heads):
        def step(masked, j, carry):
            rows = pl.ds(pl.multiple_of(j * k_rows, k_rows), k_rows)
            if masked:
                k_pos = j * k_rows + lax.broadcasted_iota(jnp.int32, (1, k_rows), 1)
                seen = (k_pos <= q_pos) & (k_pos >= q_low)
            scores, out = [], []
            for h in range(heads):
                s = lax.dot_general(q_ref[h], k_ref[h, rows, :], (((1,), (1,)), ((), ())), preferred_element_type=jnp.float32)
                scores.append(jnp.where(seen, s, -1e30) if masked else s)
            for h in range(heads):
                top, total, acc = carry[h]
                new_top = jnp.maximum(top, jnp.max(scores[h], axis=1, keepdims=True))
                decay = jnp.exp2((top - new_top) * scale)
                probs = jnp.exp2((scores[h] - new_top) * scale)
                total = total * decay + jnp.sum(probs, axis=1, keepdims=True)
                acc = acc * decay + jnp.dot(probs.astype(jnp.bfloat16), v_ref[h, rows, :], preferred_element_type=jnp.float32)
                out.append((new_top, total, acc))
            return tuple(out)

        carry = tuple((jnp.full((q_rows, 1), -1e30, jnp.float32), jnp.zeros((q_rows, 1), jnp.float32), jnp.zeros((q_rows, HEAD_DIM), jnp.float32)) for _ in range(heads))
        carry = lax.fori_loop(first, inner, functools.partial(step, True), carry)
        carry = lax.fori_loop(inner, diag, functools.partial(step, False), carry)
        carry = lax.fori_loop(diag, last + 1, functools.partial(step, True), carry)
        for h in range(heads):
            _, total, acc = carry[h]
            o_ref[h] = (acc / total).astype(jnp.bfloat16)

    for heads in range(1, slots + 1):
        pl.when(info_ref[0] == heads)(functools.partial(run, heads))


def attention(info, qkv, cuts, q_rows, k_rows):
    slots, _, group, tokens, _ = qkv.shape
    seq = group * tokens
    flat = qkv.reshape(slots, 3, seq, HEAD_DIM)

    def whole(part):
        return pl.BlockSpec((slots, None, seq, HEAD_DIM), lambda i, info: (0, part, 0, 0))

    return pl.pallas_call(
        functools.partial(attention_kernel, q_rows, k_rows, cuts),
        grid_spec=pltpu.PrefetchScalarGridSpec(
            num_scalar_prefetch=1,
            grid=(seq // q_rows,),
            in_specs=[pl.BlockSpec((slots, None, q_rows, HEAD_DIM), lambda i, info: (0, 0, i, 0)), whole(1), whole(2)],
            out_specs=pl.BlockSpec((slots, q_rows, HEAD_DIM), lambda i, info: (0, i, 0)),
        ),
        out_shape=jax.ShapeDtypeStruct((slots, seq, HEAD_DIM), jnp.bfloat16),
        compiler_params=pltpu.CompilerParams(vmem_limit_bytes=VMEM_LIMIT),
        cost_estimate=pl.CostEstimate(flops=4 * seq * seq * HEAD_DIM, bytes_accessed=8 * seq * HEAD_DIM * slots, transcendentals=seq * seq // 2),
        name="attention",
    )(info, flat, flat, flat).reshape(slots, group, tokens, HEAD_DIM)


def out_send_kernel(group, heads, o_ref, attn_ref, send_sem, recv_sem, own_sem):
    me = lax.axis_index("sp")
    mine = first_head(me, group, heads)
    count = first_head(me + 1, group, heads) - mine
    slots = o_ref.shape[0]
    greet_group(group, me)

    def hop(k):
        step = k // 2
        return (me + group // 2 + step - (k % 2) * (2 * step + 1) + group) % group

    def out_copy(slot, k):
        head = mine + slot
        return pltpu.make_async_remote_copy(
            src_ref=o_ref.at[slot, hop(k)],
            dst_ref=attn_ref.at[head],
            send_sem=send_sem.at[slot, k],
            recv_sem=recv_sem.at[head],
            device_id={"sp": hop(k)},
            device_id_type=MESH,
        )

    def own_copy(slot):
        return pltpu.make_async_copy(o_ref.at[slot, me], attn_ref.at[mine + slot], own_sem.at[slot])

    for slot in range(slots):

        @pl.when(slot < count)
        def _():
            for k in range(group - 1):
                out_copy(slot, k).start()
            own_copy(slot).start()

    for slot in range(slots):

        @pl.when(slot < count)
        def _():
            for k in range(group - 1):
                out_copy(slot, k).wait_send()
            own_copy(slot).wait()

    def landed(head, carry):
        @pl.when(owner_of(head, group, heads) != me)
        def _():
            block = attn_ref.at[head]
            pltpu.make_async_copy(block, block, recv_sem.at[head]).wait()

        return carry

    lax.fori_loop(0, heads, landed, 0)


def out_send(group, heads, o_heads):
    slots, _, tokens, _ = o_heads.shape
    hbm = pl.BlockSpec(memory_space=pl.ANY)
    return pl.pallas_call(
        functools.partial(out_send_kernel, group, heads),
        out_shape=jax.ShapeDtypeStruct((heads, tokens, HEAD_DIM), jnp.bfloat16),
        in_specs=[pl.BlockSpec(memory_space=pltpu.VMEM)],
        out_specs=hbm,
        scratch_shapes=[
            pltpu.SemaphoreType.DMA((slots, group - 1)),
            pltpu.SemaphoreType.DMA((heads,)),
            pltpu.SemaphoreType.DMA((slots,)),
        ],
        compiler_params=pltpu.CompilerParams(collective_id=1, has_side_effects=True),
        name="out_send",
    )(o_heads)


def place_rows_kernel(group, pieces, merged_ref, slots_ref, embeds_ref, gain_ref, h_ref, a_ref, rows, slots, total, hits, slot_send, slot_recv, ring_send, ring_recv, pair_send, pair_recv):
    me = lax.axis_index("sp")
    core = me % 2
    way = 2 - 4 * core
    ahead = (me + way + group) % group
    other = me + 1 - 2 * core
    hops = group // 2
    count = merged_ref.shape[0] // pieces
    greet_group(group, me)

    def origin(dev, step):
        return (dev - (2 - 4 * (dev % 2)) * step + 2 * group * group) % group

    def slot_copy(k):
        return pltpu.make_async_remote_copy(
            src_ref=slots_ref, dst_ref=slots.at[me], send_sem=slot_send.at[k], recv_sem=slot_recv.at[me],
            device_id={"sp": lax.rem(me + k, group)}, device_id_type=MESH,
        )

    def block(ref, step, piece):
        return ref.at[origin(me, step), pl.ds(piece * count, count)]

    def source(step, piece):
        return merged_ref.at[pl.ds(piece * count, count)] if step == 0 else block(rows, step, piece)

    def ring_copy(step, piece):
        return pltpu.make_async_remote_copy(
            src_ref=source(step, piece), dst_ref=block(rows, step, piece), send_sem=ring_send.at[step, piece],
            recv_sem=ring_recv.at[step, piece], device_id={"sp": ahead}, device_id_type=MESH,
        )

    def pair_copy(step, piece):
        return pltpu.make_async_remote_copy(
            src_ref=source(step, piece), dst_ref=block(rows, step, piece), send_sem=pair_send.at[step, piece],
            recv_sem=pair_recv.at[step, piece], device_id={"sp": other}, device_id_type=MESH,
        )

    for k in range(1, group):
        slot_copy(k).start()
    for piece in range(pieces):
        ring_copy(0, piece).start()
        pair_copy(0, piece).start()
    slots[me] = slots_ref[...]
    total[...] = jnp.zeros_like(total)
    hits[...] = jnp.zeros_like(hits)
    tokens = embeds_ref.shape[0]

    def place(dev, values):
        wanted = me * tokens + lax.broadcasted_iota(jnp.int32, (tokens, 1), 0)
        pick = jnp.where(slots[dev] == wanted, 1.0, 0.0)
        hits[...] += pick
        total[...] += jnp.dot(pick.astype(jnp.bfloat16), values, preferred_element_type=jnp.float32)

    for k in range(1, group):
        dev = lax.rem(me + k, group)
        pltpu.make_async_copy(slots.at[dev], slots.at[dev], slot_recv.at[dev]).wait()
    place(me, merged_ref[...])
    for step in range(hops):
        if step > 0:
            for piece in range(pieces):
                landed = block(rows, step, piece)
                pltpu.make_async_copy(landed, landed, ring_recv.at[step - 1, piece]).wait()
                if step < hops - 1:
                    ring_copy(step, piece).start()
                pair_copy(step, piece).start()
            place(origin(me, step), rows[origin(me, step)])
        theirs = origin(other, step)
        for piece in range(pieces):
            landed = rows.at[theirs, pl.ds(piece * count, count)]
            pltpu.make_async_copy(landed, landed, pair_recv.at[step, piece]).wait()
        place(theirs, rows[theirs])
    found = jnp.max(hits[...], axis=1, keepdims=True) > 0.0
    h_zero = jnp.where(found, total[...].astype(jnp.bfloat16), embeds_ref[...])
    h_ref[...] = h_zero
    a_ref[...] = rms_norm(h_zero, gain_ref[...])
    for k in range(1, group):
        slot_copy(k).wait_send()
    for step in range(hops):
        for piece in range(pieces):
            if step < hops - 1:
                ring_copy(step, piece).wait_send()
            pair_copy(step, piece).wait_send()


def place_rows(group, merged, dest_slot, embeds, gain):
    rows, width = merged.shape
    tokens = embeds.shape[0]
    pieces = 4
    hops = group // 2
    vmem = pl.BlockSpec(memory_space=pltpu.VMEM)
    out = jax.ShapeDtypeStruct((tokens, width), jnp.bfloat16)
    return pl.pallas_call(
        functools.partial(place_rows_kernel, group, pieces),
        out_shape=(out, out),
        in_specs=[vmem] * 4,
        out_specs=(vmem, vmem),
        scratch_shapes=[
            pltpu.VMEM((group, rows, width), jnp.bfloat16),
            pltpu.VMEM((group, 1, rows), jnp.int32),
            pltpu.VMEM((tokens, width), jnp.float32),
            pltpu.VMEM((tokens, rows), jnp.float32),
            pltpu.SemaphoreType.DMA((group,)),
            pltpu.SemaphoreType.DMA((group,)),
            pltpu.SemaphoreType.DMA((hops, pieces)),
            pltpu.SemaphoreType.DMA((hops, pieces)),
            pltpu.SemaphoreType.DMA((hops, pieces)),
            pltpu.SemaphoreType.DMA((hops, pieces)),
        ],
        compiler_params=pltpu.CompilerParams(collective_id=2, has_side_effects=True, vmem_limit_bytes=VMEM_LIMIT),
        name="place_rows",
    )(merged, dest_slot.reshape(1, rows), embeds, gain.reshape(1, width))


def mlp_kernel(o_cols, chunk, attn_ref, h_ref, gain_ref, wo_ref, wg_ref, wu_ref, wd_ref, out_ref, attn, h_one, normed, total, wo, wg, wu, wd, o_sem, f_sem):
    heads, _, dim = attn_ref.shape
    width = h_ref.shape[1]
    o_steps, steps = width // o_cols, wg_ref.shape[1] // chunk

    def o_copy(i):
        return pltpu.make_async_copy(wo_ref.at[:, pl.ds(i * o_cols, o_cols)], wo.at[i % 2], o_sem.at[i % 2])

    def f_copies(i):
        b = i % 2
        cols = pl.ds(pl.multiple_of(i * chunk, 128), chunk)
        return [
            pltpu.make_async_copy(wg_ref.at[:, cols], wg.at[b], f_sem.at[b, 0]),
            pltpu.make_async_copy(wu_ref.at[:, cols], wu.at[b], f_sem.at[b, 1]),
            pltpu.make_async_copy(wd_ref.at[cols, :], wd.at[b], f_sem.at[b, 2]),
        ]

    o_copy(0).start()
    o_copy(1).start()
    for h in range(heads):
        attn[:, h * dim:(h + 1) * dim] = attn_ref[h]
    for i in range(o_steps):
        o_copy(i).wait()
        cols = slice(i * o_cols, (i + 1) * o_cols)
        part = jnp.dot(attn[...], wo[i % 2], preferred_element_type=jnp.float32)
        h_one[:, cols] = (h_ref[:, cols].astype(jnp.float32) + part).astype(jnp.bfloat16)
        if i + 2 < o_steps:
            o_copy(i + 2).start()
        if i == o_steps - 3:
            for c in f_copies(0):
                c.start()
    normed[...] = rms_norm(h_one[...], gain_ref[...])
    total[...] = h_one[...].astype(jnp.float32)

    def step(i, carry):
        b = i % 2

        @pl.when(i + 1 < steps)
        def _():
            for c in f_copies(i + 1):
                c.start()

        gate_copy, up_copy, down_copy = f_copies(i)
        gate_copy.wait()
        up_copy.wait()
        gate_pre = jnp.dot(normed[...], wg[b], preferred_element_type=jnp.float32)
        up_pre = jnp.dot(normed[...], wu[b], preferred_element_type=jnp.float32)
        activated = (jax.nn.silu(gate_pre) * up_pre).astype(jnp.bfloat16)
        down_copy.wait()
        total[...] += jnp.dot(activated, wd[b], preferred_element_type=jnp.float32)
        return carry

    lax.fori_loop(0, steps, step, 0)
    out_ref[...] = total[...].astype(jnp.bfloat16)


def mlp(attn, h_zero, gain, w_o, w_gate, w_up, w_down):
    heads, tokens, dim = attn.shape
    width, ffn = w_gate.shape
    o_cols = width // 5
    chunk = ffn // 9
    vmem = pl.BlockSpec(memory_space=pltpu.VMEM)
    hbm = pl.BlockSpec(memory_space=pl.ANY)
    return pl.pallas_call(
        functools.partial(mlp_kernel, o_cols, chunk),
        out_shape=jax.ShapeDtypeStruct((tokens, width), jnp.bfloat16),
        in_specs=[vmem, vmem, vmem, hbm, hbm, hbm, hbm],
        out_specs=vmem,
        scratch_shapes=[
            pltpu.VMEM((tokens, heads * dim), jnp.bfloat16),
            pltpu.VMEM((tokens, width), jnp.bfloat16),
            pltpu.VMEM((tokens, width), jnp.bfloat16),
            pltpu.VMEM((tokens, width), jnp.float32),
            pltpu.VMEM((2, heads * dim, o_cols), jnp.bfloat16),
            pltpu.VMEM((2, width, chunk), jnp.bfloat16),
            pltpu.VMEM((2, width, chunk), jnp.bfloat16),
            pltpu.VMEM((2, chunk, width), jnp.bfloat16),
            pltpu.SemaphoreType.DMA((2,)),
            pltpu.SemaphoreType.DMA((2, 3)),
        ],
        compiler_params=pltpu.CompilerParams(vmem_limit_bytes=VMEM_LIMIT),
        cost_estimate=pl.CostEstimate(flops=2 * tokens * width * (3 * ffn + width), bytes_accessed=2 * width * (3 * ffn + width), transcendentals=tokens * ffn),
        name="mlp",
    )(attn, h_zero, gain.reshape(1, width), w_o, w_gate, w_up, w_down)


def solution(mesh):
    group = mesh.shape['sp']
    row_spec = P(('dp', 'sp'), None)

    def local_step(patches, embeds, dest_slot, rope_pos, cu_doc, ln_w, ln_b, w_one, b_one, w_two, b_two, norm_attn, w_q, b_q, w_k, b_k, w_v, b_v, w_o, norm_mlp, w_gate, w_up, w_down):
        tok_dev = embeds.shape[0]
        merged_dev = dest_slot.shape[0]
        heads = w_q.shape[1] // HEAD_DIM
        me = lax.axis_index('sp')
        normed = layer_norm(patches, ln_w, ln_b).reshape(merged_dev, -1)
        merged = merger_mlp(normed, w_one, b_one, w_two, b_two)
        h_zero, normed_a = place_rows(group, merged, dest_slot, embeds, norm_attn)
        cos_t, sin_t = rope_tables(rope_pos)
        biases = jnp.concatenate([b.astype(jnp.float32).reshape(heads, 1, HEAD_DIM) for b in (b_q, b_k, b_v)], axis=2)
        qkv = qkv_send(group, heads, normed_a, cos_t, sin_t, biases, w_q, w_k, w_v)
        count = first_head(me + 1, group, heads) - first_head(me, group, heads)
        cuts = cu_doc.shape[0] - 2
        info = jnp.concatenate([count.astype(jnp.int32).reshape(1), cu_doc[1:-1]])
        o_heads = attention(info, qkv, cuts, 512, 512)
        attn_out = out_send(group, heads, o_heads)
        return mlp(attn_out, h_zero, norm_mlp, w_o, w_gate, w_up, w_down)

    in_specs = (row_spec, row_spec, P(('dp', 'sp')), P(None, ('dp', 'sp')), P('dp')) + (P(),) * 18
    return jax.shard_map(local_step, mesh=mesh, in_specs=in_specs, out_specs=row_spec, check_vma=False)
```

```python
import functools

import jax
import jax.numpy as jnp
from jax import lax
from jax.experimental import pallas as pl
from jax.experimental.pallas import tpu as pltpu
from jax.sharding import PartitionSpec as P

HEAD_DIM = 128
NORM_EPS = 1e-6
ROPE_THETA = 1000000.0
MROPE_SPLIT = (16, 40)
MESH = pl.DeviceIdType.MESH
VMEM_LIMIT = 60 * 1024 * 1024


def layer_norm(values_in, gain_vec, shift_vec):
    widened = values_in.astype(jnp.float32)
    centered = widened - jnp.mean(widened, axis=-1, keepdims=True)
    spread = jnp.mean(centered * centered, axis=-1, keepdims=True)
    return (centered * lax.rsqrt(spread + NORM_EPS) * gain_vec.astype(jnp.float32) + shift_vec.astype(jnp.float32)).astype(jnp.bfloat16)


def rms_norm(values_in, gain_vec):
    widened = values_in.astype(jnp.float32)
    return (widened * lax.rsqrt(jnp.mean(widened * widened, axis=-1, keepdims=True) + NORM_EPS) * gain_vec.astype(jnp.float32)).astype(jnp.bfloat16)


def merger_mlp(grouped, w_one, b_one, w_two, b_two):
    inner = jax.nn.gelu(jnp.dot(grouped, w_one, preferred_element_type=jnp.float32) + b_one.astype(jnp.float32), approximate=False).astype(jnp.bfloat16)
    return (jnp.dot(inner, w_two, preferred_element_type=jnp.float32) + b_two.astype(jnp.float32)).astype(jnp.bfloat16)


def rope_tables(rope_pos):
    inv_freq = ROPE_THETA ** (-jnp.arange(0, HEAD_DIM, 2, dtype=jnp.float32) / HEAD_DIM)
    freq_idx = jnp.arange(HEAD_DIM // 2)[None, :]
    chosen = jnp.where(freq_idx < MROPE_SPLIT[0], rope_pos[0][:, None], jnp.where(freq_idx < MROPE_SPLIT[1], rope_pos[1][:, None], rope_pos[2][:, None]))
    angles = chosen.astype(jnp.float32) * inv_freq[None, :]
    cos_h, sin_h = jnp.cos(angles), jnp.sin(angles)
    return jnp.concatenate([cos_h, cos_h], axis=-1), jnp.concatenate([-sin_h, sin_h], axis=-1)


def first_head(dev, group, heads):
    return (dev * heads + group - 1) // group


def owner_of(head, group, heads):
    return head * group // heads


def greet_group(group, me):
    barrier = pltpu.get_barrier_semaphore()
    for k in range(1, group):
        pl.semaphore_signal(barrier, inc=1, device_id={"sp": lax.rem(me + k, group)}, device_id_type=MESH)
    pl.semaphore_wait(barrier, group - 1)


def mixer_kernel(group, heads, cuts, cu_ref, a_ref, cos_ref, sin_ref, bias_ref, wq_ref, wk_ref, wv_ref, attn_ref, wbuf, stage, land, top_ref, sum_ref, acc_ref, o_ref, w_sem, send_sem, recv_sem, own_sem, o_send, o_recv, o_own):
    me = lax.axis_index("sp")
    chips = group // 2
    my_chip = me // 2
    depth = wbuf.shape[0]
    slots = land.shape[0]
    tokens = a_ref.shape[0]
    rows = 2 * tokens
    mine = first_head(me, group, heads)
    count = first_head(me + 1, group, heads) - mine

    def head_at(p):
        step = (p + 1) // 2
        return (mine + (2 * (p % 2) - 1) * step + heads) % heads

    def weight_copies(p):
        cols = pl.ds(pl.multiple_of(head_at(p) * HEAD_DIM, HEAD_DIM), HEAD_DIM)
        slot = p % depth
        return [
            pltpu.make_async_copy(w.at[:, cols], wbuf.at[slot, :, pl.ds(n * HEAD_DIM, HEAD_DIM)], w_sem.at[slot, n])
            for n, w in enumerate((wq_ref, wk_ref, wv_ref))
        ]

    def remote(p):
        head = head_at(p)
        target = owner_of(head, group, heads)
        slot = head - first_head(target, group, heads)
        copy = pltpu.make_async_remote_copy(
            src_ref=stage.at[p],
            dst_ref=land.at[slot, me],
            send_sem=send_sem.at[p],
            recv_sem=recv_sem.at[slot, me],
            device_id={"sp": target},
            device_id_type=MESH,
        )
        local = pltpu.make_async_copy(stage.at[p], land.at[slot, me], own_sem.at[slot])
        return target, copy, local

    def send(p):
        target, copy, local = remote(p)

        @pl.when(target != me)
        def _():
            copy.start()

        @pl.when(target == me)
        def _():
            local.start()

    for p in range(depth - 1):
        for c in weight_copies(p):
            c.start()
    greet_group(group, me)

    def project(p, carry):
        @pl.when(p + depth - 1 < heads)
        def _():
            for c in weight_copies(p + depth - 1):
                c.start()

        for c in weight_copies(p):
            c.wait()
        lin = jnp.dot(a_ref[...], wbuf[p % depth], preferred_element_type=jnp.float32) + bias_ref[head_at(p)]

        @pl.when(p > 0)
        def _():
            send(p - 1)

        cos_t, sin_t = cos_ref[...], sin_ref[...]
        for n in range(3):
            part = lin[:, n * HEAD_DIM:(n + 1) * HEAD_DIM]
            if n < 2:
                part = part * cos_t + pltpu.roll(part, HEAD_DIM // 2, 1) * sin_t
            stage[p, n] = part.astype(jnp.bfloat16)
        return carry

    lax.fori_loop(0, heads, project, 0)

    def clear(c, carry):
        for slot in range(slots):
            top_ref[slot, c] = jnp.full((rows, HEAD_DIM), -1e30, jnp.float32)
            sum_ref[slot, c] = jnp.zeros((rows, HEAD_DIM), jnp.float32)
            acc_ref[slot, c] = jnp.zeros((rows, HEAD_DIM), jnp.float32)
        return carry

    send(heads - 1)
    lax.fori_loop(0, chips, clear, 0)
    scale = HEAD_DIM ** -0.5 * 1.4426950408889634

    def chip_at(t):
        step = (t + 1) // 2
        return (my_chip + (2 * (t % 2) - 1) * step + chips) % chips

    def block(slot, part, chip):
        return land[slot, pl.ds(2 * chip, 2), part].reshape(rows, HEAD_DIM)

    def attend(slot, q_chip, k_chip, causal):
        scores = lax.dot_general(block(slot, 0, q_chip), block(slot, 1, k_chip), (((1,), (1,)), ((), ())), preferred_element_type=jnp.float32)
        q_pos = q_chip * rows + lax.broadcasted_iota(jnp.int32, (rows, 1), 0)
        q_low = jnp.zeros((rows, 1), jnp.int32)
        for d in range(1, cuts + 1):
            q_low = jnp.where(q_pos >= cu_ref[d], cu_ref[d], q_low)
        k_pos = k_chip * rows + lax.broadcasted_iota(jnp.int32, (1, rows), 1)
        seen = k_pos >= q_low
        if causal:
            seen = seen & (k_pos <= q_pos)
        scores = jnp.where(seen, scores, -1e30)
        top = top_ref[slot, q_chip]
        new_top = jnp.maximum(top, jnp.max(scores, axis=1, keepdims=True))
        decay = jnp.exp2((top - new_top) * scale)
        total = sum_ref[slot, q_chip] * decay
        parts = []
        for n in range(rows // HEAD_DIM):
            probs = jnp.exp2((scores[:, n * HEAD_DIM:(n + 1) * HEAD_DIM] - new_top) * scale)
            total = total + probs
            parts.append(probs.astype(jnp.bfloat16))
        mixed = jnp.dot(jnp.concatenate(parts, axis=1), block(slot, 2, k_chip), preferred_element_type=jnp.float32)
        top_ref[slot, q_chip] = new_top
        sum_ref[slot, q_chip] = total
        acc_ref[slot, q_chip] = acc_ref[slot, q_chip] * decay + mixed

    def for_slots(action):
        lax.fori_loop(0, count, lambda slot, carry: (action(slot), carry)[1], 0)

    def wait_chip(chip):
        def one(slot):
            for core in range(2):
                dev = 2 * chip + core
                landed = land.at[slot, dev]

                @pl.when(dev != me)
                def _():
                    pltpu.make_async_copy(landed, landed, recv_sem.at[slot, dev]).wait()

                @pl.when(dev == me)
                def _():
                    pltpu.make_async_copy(landed, landed, own_sem.at[slot]).wait()

        for_slots(one)

    def pair(t, u):
        here, there = chip_at(t), chip_at(u)
        later = (here - there + chips) // chips
        q_chip = here * later + there * (1 - later)
        k_chip = there * later + here * (1 - later)
        for_slots(lambda slot: attend(slot, q_chip, k_chip, False))

    def o_copy(slot, dev):
        return pltpu.make_async_remote_copy(
            src_ref=o_ref.at[slot, dev],
            dst_ref=attn_ref.at[mine + slot],
            send_sem=o_send.at[slot, dev],
            recv_sem=o_recv.at[mine + slot],
            device_id={"sp": dev},
            device_id_type=MESH,
        )

    def o_local(slot):
        return pltpu.make_async_copy(o_ref.at[slot, me], attn_ref.at[mine + slot], o_own.at[slot])

    def finish(chip):
        def divide(slot):
            total = jnp.sum(sum_ref[slot, chip], axis=1, keepdims=True)
            out = (acc_ref[slot, chip] / total).astype(jnp.bfloat16)
            o_ref[slot, pl.ds(2 * chip, 2)] = out.reshape(2, tokens, HEAD_DIM)

        def give(slot):
            for core in range(2):
                dev = 2 * chip + core

                @pl.when(dev != me)
                def _():
                    o_copy(slot, dev).start()

                @pl.when(dev == me)
                def _():
                    o_local(slot).start()

        for_slots(divide)
        for_slots(give)

    def arrival(t, carry):
        chip = chip_at(t)
        wait_chip(chip)
        for_slots(lambda slot: attend(slot, chip, chip, True))
        lax.fori_loop(0, t, lambda u, c: (pair(t, u), c)[1], 0)
        return carry

    last = chips - 1
    far = chip_at(last)
    lax.fori_loop(0, last, arrival, 0)

    def early(u, carry):
        @pl.when(chip_at(u) < far)
        def _():
            finish(chip_at(u))

        return carry

    lax.fori_loop(0, last, early, 0)
    wait_chip(far)
    for_slots(lambda slot: attend(slot, far, far, True))

    def late(u, carry):
        pair(last, u)

        @pl.when(chip_at(u) > far)
        def _():
            finish(chip_at(u))

        return carry

    lax.fori_loop(0, last, late, 0)
    finish(far)

    def drain(p, carry):
        target, copy, _ = remote(p)

        @pl.when(target != me)
        def _():
            copy.wait_send()

        return carry

    lax.fori_loop(0, heads, drain, 0)

    def drain_out(slot):
        def one(dev, carry):
            @pl.when(dev != me)
            def _():
                o_copy(slot, dev).wait_send()

            return carry

        lax.fori_loop(0, group, one, 0)
        o_local(slot).wait()

    for_slots(drain_out)

    def landed_out(head, carry):
        @pl.when(owner_of(head, group, heads) != me)
        def _():
            back = attn_ref.at[head]
            pltpu.make_async_copy(back, back, o_recv.at[head]).wait()

        return carry

    lax.fori_loop(0, heads, landed_out, 0)


def mixer(group, heads, cu_doc, normed, cos_t, sin_t, biases, w_q, w_k, w_v):
    tokens, width = normed.shape
    slots = -(-heads // group)
    chips = group // 2
    vmem = pl.BlockSpec(memory_space=pltpu.VMEM)
    smem = pl.BlockSpec(memory_space=pltpu.SMEM)
    hbm = pl.BlockSpec(memory_space=pl.ANY)
    state = pltpu.VMEM((slots, chips, 2 * tokens, HEAD_DIM), jnp.float32)
    return pl.pallas_call(
        functools.partial(mixer_kernel, group, heads, cu_doc.shape[0] - 2),
        out_shape=jax.ShapeDtypeStruct((heads, tokens, HEAD_DIM), jnp.bfloat16),
        in_specs=[smem, vmem, vmem, vmem, vmem, hbm, hbm, hbm],
        out_specs=hbm,
        scratch_shapes=[
            pltpu.VMEM((3, width, 3 * HEAD_DIM), jnp.bfloat16),
            pltpu.VMEM((heads, 3, tokens, HEAD_DIM), jnp.bfloat16),
            pltpu.VMEM((slots, group, 3, tokens, HEAD_DIM), jnp.bfloat16),
            state,
            state,
            state,
            pltpu.VMEM((slots, group, tokens, HEAD_DIM), jnp.bfloat16),
            pltpu.SemaphoreType.DMA((3, 3)),
            pltpu.SemaphoreType.DMA((heads,)),
            pltpu.SemaphoreType.DMA((slots, group)),
            pltpu.SemaphoreType.DMA((slots,)),
            pltpu.SemaphoreType.DMA((slots, group)),
            pltpu.SemaphoreType.DMA((heads,)),
            pltpu.SemaphoreType.DMA((slots,)),
        ],
        compiler_params=pltpu.CompilerParams(collective_id=0, has_side_effects=True, vmem_limit_bytes=VMEM_LIMIT),
        cost_estimate=pl.CostEstimate(flops=2 * tokens * width * 3 * heads * HEAD_DIM, bytes_accessed=3 * width * heads * HEAD_DIM * 2, transcendentals=0),
        name="mixer",
    )(cu_doc, normed, cos_t, sin_t, biases, w_q, w_k, w_v)


def place_rows_kernel(group, pieces, merged_ref, slots_ref, embeds_ref, gain_ref, h_ref, a_ref, rows, slots, total, hits, slot_send, slot_recv, ring_send, ring_recv, pair_send, pair_recv):
    me = lax.axis_index("sp")
    core = me % 2
    way = 2 - 4 * core
    ahead = (me + way + group) % group
    other = me + 1 - 2 * core
    hops = group // 2
    count = merged_ref.shape[0] // pieces
    greet_group(group, me)

    def origin(dev, step):
        return (dev - (2 - 4 * (dev % 2)) * step + 2 * group * group) % group

    def slot_copy(k):
        return pltpu.make_async_remote_copy(
            src_ref=slots_ref, dst_ref=slots.at[me], send_sem=slot_send.at[k], recv_sem=slot_recv.at[me],
            device_id={"sp": lax.rem(me + k, group)}, device_id_type=MESH,
        )

    def block(ref, step, piece):
        return ref.at[origin(me, step), pl.ds(piece * count, count)]

    def source(step, piece):
        return merged_ref.at[pl.ds(piece * count, count)] if step == 0 else block(rows, step, piece)

    def ring_copy(step, piece):
        return pltpu.make_async_remote_copy(
            src_ref=source(step, piece), dst_ref=block(rows, step, piece), send_sem=ring_send.at[step, piece],
            recv_sem=ring_recv.at[step, piece], device_id={"sp": ahead}, device_id_type=MESH,
        )

    def pair_copy(step, piece):
        return pltpu.make_async_remote_copy(
            src_ref=source(step, piece), dst_ref=block(rows, step, piece), send_sem=pair_send.at[step, piece],
            recv_sem=pair_recv.at[step, piece], device_id={"sp": other}, device_id_type=MESH,
        )

    for k in range(1, group):
        slot_copy(k).start()
    for piece in range(pieces):
        ring_copy(0, piece).start()
        pair_copy(0, piece).start()
    slots[me] = slots_ref[...]
    total[...] = jnp.zeros_like(total)
    hits[...] = jnp.zeros_like(hits)
    tokens = embeds_ref.shape[0]

    def place(dev, values):
        wanted = me * tokens + lax.broadcasted_iota(jnp.int32, (tokens, 1), 0)
        pick = jnp.where(slots[dev] == wanted, 1.0, 0.0)
        hits[...] += pick
        total[...] += jnp.dot(pick.astype(jnp.bfloat16), values, preferred_element_type=jnp.float32)

    for k in range(1, group):
        dev = lax.rem(me + k, group)
        pltpu.make_async_copy(slots.at[dev], slots.at[dev], slot_recv.at[dev]).wait()
    place(me, merged_ref[...])
    for step in range(hops):
        if step > 0:
            for piece in range(pieces):
                landed = block(rows, step, piece)
                pltpu.make_async_copy(landed, landed, ring_recv.at[step - 1, piece]).wait()
                if step < hops - 1:
                    ring_copy(step, piece).start()
                pair_copy(step, piece).start()
            place(origin(me, step), rows[origin(me, step)])
        theirs = origin(other, step)
        for piece in range(pieces):
            landed = rows.at[theirs, pl.ds(piece * count, count)]
            pltpu.make_async_copy(landed, landed, pair_recv.at[step, piece]).wait()
        place(theirs, rows[theirs])
    found = jnp.max(hits[...], axis=1, keepdims=True) > 0.0
    h_zero = jnp.where(found, total[...].astype(jnp.bfloat16), embeds_ref[...])
    h_ref[...] = h_zero
    a_ref[...] = rms_norm(h_zero, gain_ref[...])
    for k in range(1, group):
        slot_copy(k).wait_send()
    for step in range(hops):
        for piece in range(pieces):
            if step < hops - 1:
                ring_copy(step, piece).wait_send()
            pair_copy(step, piece).wait_send()


def place_rows(group, merged, dest_slot, embeds, gain):
    rows, width = merged.shape
    tokens = embeds.shape[0]
    pieces = 4
    hops = group // 2
    vmem = pl.BlockSpec(memory_space=pltpu.VMEM)
    out = jax.ShapeDtypeStruct((tokens, width), jnp.bfloat16)
    return pl.pallas_call(
        functools.partial(place_rows_kernel, group, pieces),
        out_shape=(out, out),
        in_specs=[vmem] * 4,
        out_specs=(vmem, vmem),
        scratch_shapes=[
            pltpu.VMEM((group, rows, width), jnp.bfloat16),
            pltpu.VMEM((group, 1, rows), jnp.int32),
            pltpu.VMEM((tokens, width), jnp.float32),
            pltpu.VMEM((tokens, rows), jnp.float32),
            pltpu.SemaphoreType.DMA((group,)),
            pltpu.SemaphoreType.DMA((group,)),
            pltpu.SemaphoreType.DMA((hops, pieces)),
            pltpu.SemaphoreType.DMA((hops, pieces)),
            pltpu.SemaphoreType.DMA((hops, pieces)),
            pltpu.SemaphoreType.DMA((hops, pieces)),
        ],
        compiler_params=pltpu.CompilerParams(collective_id=2, has_side_effects=True, vmem_limit_bytes=VMEM_LIMIT),
        name="place_rows",
    )(merged, dest_slot.reshape(1, rows), embeds, gain.reshape(1, width))


def mlp_kernel(o_cols, chunk, attn_ref, h_ref, gain_ref, wo_ref, wg_ref, wu_ref, wd_ref, out_ref, attn, h_one, normed, total, wo, wg, wu, wd, o_sem, f_sem):
    heads, _, dim = attn_ref.shape
    width = h_ref.shape[1]
    o_steps, steps = width // o_cols, wg_ref.shape[1] // chunk

    def o_copy(i):
        return pltpu.make_async_copy(wo_ref.at[:, pl.ds(i * o_cols, o_cols)], wo.at[i % 2], o_sem.at[i % 2])

    def f_copies(i):
        b = i % 2
        cols = pl.ds(pl.multiple_of(i * chunk, 128), chunk)
        return [
            pltpu.make_async_copy(wg_ref.at[:, cols], wg.at[b], f_sem.at[b, 0]),
            pltpu.make_async_copy(wu_ref.at[:, cols], wu.at[b], f_sem.at[b, 1]),
            pltpu.make_async_copy(wd_ref.at[cols, :], wd.at[b], f_sem.at[b, 2]),
        ]

    o_copy(0).start()
    o_copy(1).start()
    for h in range(heads):
        attn[:, h * dim:(h + 1) * dim] = attn_ref[h]
    for i in range(o_steps):
        o_copy(i).wait()
        cols = slice(i * o_cols, (i + 1) * o_cols)
        part = jnp.dot(attn[...], wo[i % 2], preferred_element_type=jnp.float32)
        h_one[:, cols] = (h_ref[:, cols].astype(jnp.float32) + part).astype(jnp.bfloat16)
        if i + 2 < o_steps:
            o_copy(i + 2).start()
        if i == o_steps - 3:
            for c in f_copies(0):
                c.start()
    normed[...] = rms_norm(h_one[...], gain_ref[...])
    total[...] = h_one[...].astype(jnp.float32)

    def step(i, carry):
        b = i % 2

        @pl.when(i + 1 < steps)
        def _():
            for c in f_copies(i + 1):
                c.start()

        gate_copy, up_copy, down_copy = f_copies(i)
        gate_copy.wait()
        up_copy.wait()
        gate_pre = jnp.dot(normed[...], wg[b], preferred_element_type=jnp.float32)
        up_pre = jnp.dot(normed[...], wu[b], preferred_element_type=jnp.float32)
        activated = (jax.nn.silu(gate_pre) * up_pre).astype(jnp.bfloat16)
        down_copy.wait()
        total[...] += jnp.dot(activated, wd[b], preferred_element_type=jnp.float32)
        return carry

    lax.fori_loop(0, steps, step, 0)
    out_ref[...] = total[...].astype(jnp.bfloat16)


def mlp(attn, h_zero, gain, w_o, w_gate, w_up, w_down):
    heads, tokens, dim = attn.shape
    width, ffn = w_gate.shape
    o_cols = width // 5
    chunk = ffn // 9
    vmem = pl.BlockSpec(memory_space=pltpu.VMEM)
    hbm = pl.BlockSpec(memory_space=pl.ANY)
    return pl.pallas_call(
        functools.partial(mlp_kernel, o_cols, chunk),
        out_shape=jax.ShapeDtypeStruct((tokens, width), jnp.bfloat16),
        in_specs=[vmem, vmem, vmem, hbm, hbm, hbm, hbm],
        out_specs=vmem,
        scratch_shapes=[
            pltpu.VMEM((tokens, heads * dim), jnp.bfloat16),
            pltpu.VMEM((tokens, width), jnp.bfloat16),
            pltpu.VMEM((tokens, width), jnp.bfloat16),
            pltpu.VMEM((tokens, width), jnp.float32),
            pltpu.VMEM((2, heads * dim, o_cols), jnp.bfloat16),
            pltpu.VMEM((2, width, chunk), jnp.bfloat16),
            pltpu.VMEM((2, width, chunk), jnp.bfloat16),
            pltpu.VMEM((2, chunk, width), jnp.bfloat16),
            pltpu.SemaphoreType.DMA((2,)),
            pltpu.SemaphoreType.DMA((2, 3)),
        ],
        compiler_params=pltpu.CompilerParams(vmem_limit_bytes=VMEM_LIMIT),
        cost_estimate=pl.CostEstimate(flops=2 * tokens * width * (3 * ffn + width), bytes_accessed=2 * width * (3 * ffn + width), transcendentals=tokens * ffn),
        name="mlp",
    )(attn, h_zero, gain.reshape(1, width), w_o, w_gate, w_up, w_down)


def solution(mesh):
    group = mesh.shape['sp']
    row_spec = P(('dp', 'sp'), None)

    def local_step(patches, embeds, dest_slot, rope_pos, cu_doc, ln_w, ln_b, w_one, b_one, w_two, b_two, norm_attn, w_q, b_q, w_k, b_k, w_v, b_v, w_o, norm_mlp, w_gate, w_up, w_down):
        tok_dev = embeds.shape[0]
        merged_dev = dest_slot.shape[0]
        heads = w_q.shape[1] // HEAD_DIM
        normed = layer_norm(patches, ln_w, ln_b).reshape(merged_dev, -1)
        merged = merger_mlp(normed, w_one, b_one, w_two, b_two)
        h_zero, normed_a = place_rows(group, merged, dest_slot, embeds, norm_attn)
        cos_t, sin_t = rope_tables(rope_pos)
        biases = jnp.concatenate([b.astype(jnp.float32).reshape(heads, 1, HEAD_DIM) for b in (b_q, b_k, b_v)], axis=2)
        attn_out = mixer(group, heads, cu_doc, normed_a, cos_t, sin_t, biases, w_q, w_k, w_v)
        return mlp(attn_out, h_zero, norm_mlp, w_o, w_gate, w_up, w_down)

    in_specs = (row_spec, row_spec, P(('dp', 'sp')), P(None, ('dp', 'sp')), P('dp')) + (P(),) * 18
    return jax.shard_map(local_step, mesh=mesh, in_specs=in_specs, out_specs=row_spec, check_vma=False)
```

```python
import functools

import jax
import jax.numpy as jnp
from jax import lax
from jax.experimental import pallas as pl
from jax.experimental.pallas import tpu as pltpu
from jax.sharding import PartitionSpec as P

HEAD_DIM = 128
NORM_EPS = 1e-6
ROPE_THETA = 1000000.0
MROPE_SPLIT = (16, 40)
MESH = pl.DeviceIdType.MESH
VMEM_LIMIT = 60 * 1024 * 1024


def layer_norm(values_in, gain_vec, shift_vec):
    widened = values_in.astype(jnp.float32)
    centered = widened - jnp.mean(widened, axis=-1, keepdims=True)
    spread = jnp.mean(centered * centered, axis=-1, keepdims=True)
    return (centered * lax.rsqrt(spread + NORM_EPS) * gain_vec.astype(jnp.float32) + shift_vec.astype(jnp.float32)).astype(jnp.bfloat16)


def rms_norm(values_in, gain_vec):
    widened = values_in.astype(jnp.float32)
    return (widened * lax.rsqrt(jnp.mean(widened * widened, axis=-1, keepdims=True) + NORM_EPS) * gain_vec.astype(jnp.float32)).astype(jnp.bfloat16)


def rope_tables(rope_pos):
    inv_freq = ROPE_THETA ** (-jnp.arange(0, HEAD_DIM, 2, dtype=jnp.float32) / HEAD_DIM)
    freq_idx = jnp.arange(HEAD_DIM // 2)[None, :]
    chosen = jnp.where(freq_idx < MROPE_SPLIT[0], rope_pos[0][:, None], jnp.where(freq_idx < MROPE_SPLIT[1], rope_pos[1][:, None], rope_pos[2][:, None]))
    angles = chosen.astype(jnp.float32) * inv_freq[None, :]
    cos_h, sin_h = jnp.cos(angles), jnp.sin(angles)
    return jnp.concatenate([cos_h, cos_h], axis=-1), jnp.concatenate([-sin_h, sin_h], axis=-1)


def first_head(dev, group, heads):
    return (dev * heads + group - 1) // group


def owner_of(head, group, heads):
    return head * group // heads


def greet_group(group, me):
    barrier = pltpu.get_barrier_semaphore()
    for k in range(1, group):
        pl.semaphore_signal(barrier, inc=1, device_id={"sp": lax.rem(me + k, group)}, device_id_type=MESH)
    pl.semaphore_wait(barrier, group - 1)


def mixer_kernel(group, heads, cuts, cu_ref, a_ref, cos_ref, sin_ref, bias_ref, wq_ref, wk_ref, wv_ref, attn_ref, wbuf, stage, land, top_ref, sum_ref, acc_ref, o_ref, w_sem, send_sem, recv_sem, own_sem, o_send, o_recv, o_own):
    me = lax.axis_index("sp")
    chips = group // 2
    my_chip = me // 2
    depth = wbuf.shape[0]
    slots = land.shape[0]
    tokens = a_ref.shape[0]
    rows = 2 * tokens
    mine = first_head(me, group, heads)
    count = first_head(me + 1, group, heads) - mine

    def head_at(p):
        step = (p + 1) // 2
        return (mine + (2 * (p % 2) - 1) * step + heads) % heads

    def weight_copies(p):
        cols = pl.ds(pl.multiple_of(head_at(p) * HEAD_DIM, HEAD_DIM), HEAD_DIM)
        slot = p % depth
        return [
            pltpu.make_async_copy(w.at[:, cols], wbuf.at[slot, :, pl.ds(n * HEAD_DIM, HEAD_DIM)], w_sem.at[slot, n])
            for n, w in enumerate((wq_ref, wk_ref, wv_ref))
        ]

    def remote(p):
        head = head_at(p)
        target = owner_of(head, group, heads)
        slot = head - first_head(target, group, heads)
        copy = pltpu.make_async_remote_copy(
            src_ref=stage.at[p],
            dst_ref=land.at[slot, me],
            send_sem=send_sem.at[p],
            recv_sem=recv_sem.at[slot, me],
            device_id={"sp": target},
            device_id_type=MESH,
        )
        local = pltpu.make_async_copy(stage.at[p], land.at[slot, me], own_sem.at[slot])
        return target, copy, local

    def send(p):
        target, copy, local = remote(p)

        @pl.when(target != me)
        def _():
            copy.start()

        @pl.when(target == me)
        def _():
            local.start()

    for p in range(depth - 1):
        for c in weight_copies(p):
            c.start()
    greet_group(group, me)

    def project(p, carry):
        @pl.when(p + depth - 1 < heads)
        def _():
            for c in weight_copies(p + depth - 1):
                c.start()

        for c in weight_copies(p):
            c.wait()
        lin = jnp.dot(a_ref[...], wbuf[p % depth], preferred_element_type=jnp.float32) + bias_ref[head_at(p)]

        @pl.when(p > 0)
        def _():
            send(p - 1)

        cos_t, sin_t = cos_ref[...], sin_ref[...]
        for n in range(3):
            part = lin[:, n * HEAD_DIM:(n + 1) * HEAD_DIM]
            if n < 2:
                part = part * cos_t + pltpu.roll(part, HEAD_DIM // 2, 1) * sin_t
            stage[p, n] = part.astype(jnp.bfloat16)
        return carry

    lax.fori_loop(0, heads, project, 0)

    def clear(c, carry):
        for slot in range(slots):
            top_ref[slot, c] = jnp.full((rows, HEAD_DIM), -1e30, jnp.float32)
            sum_ref[slot, c] = jnp.zeros((rows, HEAD_DIM), jnp.float32)
            acc_ref[slot, c] = jnp.zeros((rows, HEAD_DIM), jnp.float32)
        return carry

    send(heads - 1)
    lax.fori_loop(0, chips, clear, 0)
    scale = HEAD_DIM ** -0.5 * 1.4426950408889634

    def chip_at(t):
        step = (t + 1) // 2
        return (my_chip + (2 * (t % 2) - 1) * step + chips) % chips

    def block(slot, part, chip):
        return land[slot, pl.ds(2 * chip, 2), part].reshape(rows, HEAD_DIM)

    def attend(slot, q_chip, k_chip, causal):
        scores = lax.dot_general(block(slot, 0, q_chip), block(slot, 1, k_chip), (((1,), (1,)), ((), ())), preferred_element_type=jnp.float32)
        q_pos = q_chip * rows + lax.broadcasted_iota(jnp.int32, (rows, 1), 0)
        q_low = jnp.zeros((rows, 1), jnp.int32)
        for d in range(1, cuts + 1):
            q_low = jnp.where(q_pos >= cu_ref[d], cu_ref[d], q_low)
        k_pos = k_chip * rows + lax.broadcasted_iota(jnp.int32, (1, rows), 1)
        seen = k_pos >= q_low
        if causal:
            seen = seen & (k_pos <= q_pos)
        scores = jnp.where(seen, scores, -1e30)
        top = top_ref[slot, q_chip]
        new_top = jnp.maximum(top, jnp.max(scores, axis=1, keepdims=True))
        decay = jnp.exp2((top - new_top) * scale)
        total = sum_ref[slot, q_chip] * decay
        parts = []
        for n in range(rows // HEAD_DIM):
            probs = jnp.exp2((scores[:, n * HEAD_DIM:(n + 1) * HEAD_DIM] - new_top) * scale)
            total = total + probs
            parts.append(probs.astype(jnp.bfloat16))
        mixed = jnp.dot(jnp.concatenate(parts, axis=1), block(slot, 2, k_chip), preferred_element_type=jnp.float32)
        top_ref[slot, q_chip] = new_top
        sum_ref[slot, q_chip] = total
        acc_ref[slot, q_chip] = acc_ref[slot, q_chip] * decay + mixed

    def for_slots(action):
        lax.fori_loop(0, count, lambda slot, carry: (action(slot), carry)[1], 0)

    def wait_chip(chip):
        def one(slot):
            for core in range(2):
                dev = 2 * chip + core
                landed = land.at[slot, dev]

                @pl.when(dev != me)
                def _():
                    pltpu.make_async_copy(landed, landed, recv_sem.at[slot, dev]).wait()

                @pl.when(dev == me)
                def _():
                    pltpu.make_async_copy(landed, landed, own_sem.at[slot]).wait()

        for_slots(one)

    def pair(t, u):
        here, there = chip_at(t), chip_at(u)
        later = (here - there + chips) // chips
        q_chip = here * later + there * (1 - later)
        k_chip = there * later + here * (1 - later)
        for_slots(lambda slot: attend(slot, q_chip, k_chip, False))

    def o_copy(slot, dev):
        return pltpu.make_async_remote_copy(
            src_ref=o_ref.at[slot, dev],
            dst_ref=attn_ref.at[mine + slot],
            send_sem=o_send.at[slot, dev],
            recv_sem=o_recv.at[mine + slot],
            device_id={"sp": dev},
            device_id_type=MESH,
        )

    def o_local(slot):
        return pltpu.make_async_copy(o_ref.at[slot, me], attn_ref.at[mine + slot], o_own.at[slot])

    def finish(chip):
        def divide(slot):
            total = jnp.sum(sum_ref[slot, chip], axis=1, keepdims=True)
            out = (acc_ref[slot, chip] / total).astype(jnp.bfloat16)
            o_ref[slot, pl.ds(2 * chip, 2)] = out.reshape(2, tokens, HEAD_DIM)

        def give(slot):
            for core in range(2):
                dev = 2 * chip + core

                @pl.when(dev != me)
                def _():
                    o_copy(slot, dev).start()

                @pl.when(dev == me)
                def _():
                    o_local(slot).start()

        for_slots(divide)
        for_slots(give)

    def arrival(t, carry):
        chip = chip_at(t)
        wait_chip(chip)
        for_slots(lambda slot: attend(slot, chip, chip, True))
        lax.fori_loop(0, t, lambda u, c: (pair(t, u), c)[1], 0)
        return carry

    last = chips - 1
    far = chip_at(last)
    lax.fori_loop(0, last, arrival, 0)

    def early(u, carry):
        @pl.when(chip_at(u) < far)
        def _():
            finish(chip_at(u))

        return carry

    lax.fori_loop(0, last, early, 0)
    wait_chip(far)
    for_slots(lambda slot: attend(slot, far, far, True))

    def late(u, carry):
        pair(last, u)

        @pl.when(chip_at(u) > far)
        def _():
            finish(chip_at(u))

        return carry

    lax.fori_loop(0, last, late, 0)
    finish(far)

    def drain(p, carry):
        target, copy, _ = remote(p)

        @pl.when(target != me)
        def _():
            copy.wait_send()

        return carry

    lax.fori_loop(0, heads, drain, 0)

    def drain_out(slot):
        def one(dev, carry):
            @pl.when(dev != me)
            def _():
                o_copy(slot, dev).wait_send()

            return carry

        lax.fori_loop(0, group, one, 0)
        o_local(slot).wait()

    for_slots(drain_out)

    def landed_out(head, carry):
        @pl.when(owner_of(head, group, heads) != me)
        def _():
            back = attn_ref.at[head]
            pltpu.make_async_copy(back, back, o_recv.at[head]).wait()

        return carry

    lax.fori_loop(0, heads, landed_out, 0)


def mixer(group, heads, cu_doc, normed, cos_t, sin_t, biases, w_q, w_k, w_v):
    tokens, width = normed.shape
    slots = -(-heads // group)
    chips = group // 2
    vmem = pl.BlockSpec(memory_space=pltpu.VMEM)
    smem = pl.BlockSpec(memory_space=pltpu.SMEM)
    hbm = pl.BlockSpec(memory_space=pl.ANY)
    state = pltpu.VMEM((slots, chips, 2 * tokens, HEAD_DIM), jnp.float32)
    return pl.pallas_call(
        functools.partial(mixer_kernel, group, heads, cu_doc.shape[0] - 2),
        out_shape=jax.ShapeDtypeStruct((heads, tokens, HEAD_DIM), jnp.bfloat16),
        in_specs=[smem, vmem, vmem, vmem, vmem, hbm, hbm, hbm],
        out_specs=hbm,
        scratch_shapes=[
            pltpu.VMEM((3, width, 3 * HEAD_DIM), jnp.bfloat16),
            pltpu.VMEM((heads, 3, tokens, HEAD_DIM), jnp.bfloat16),
            pltpu.VMEM((slots, group, 3, tokens, HEAD_DIM), jnp.bfloat16),
            state,
            state,
            state,
            pltpu.VMEM((slots, group, tokens, HEAD_DIM), jnp.bfloat16),
            pltpu.SemaphoreType.DMA((3, 3)),
            pltpu.SemaphoreType.DMA((heads,)),
            pltpu.SemaphoreType.DMA((slots, group)),
            pltpu.SemaphoreType.DMA((slots,)),
            pltpu.SemaphoreType.DMA((slots, group)),
            pltpu.SemaphoreType.DMA((heads,)),
            pltpu.SemaphoreType.DMA((slots,)),
        ],
        compiler_params=pltpu.CompilerParams(collective_id=0, has_side_effects=True, vmem_limit_bytes=VMEM_LIMIT),
        cost_estimate=pl.CostEstimate(flops=2 * tokens * width * 3 * heads * HEAD_DIM, bytes_accessed=3 * width * heads * HEAD_DIM * 2, transcendentals=0),
        name="mixer",
    )(cu_doc, normed, cos_t, sin_t, biases, w_q, w_k, w_v)


def merge_place_kernel(group, patch_ref, lnw_ref, lnb_ref, b1_ref, b2_ref, slots_ref, embeds_ref, gain_ref, w1_ref, w2_ref, h_ref, a_ref, z, wbuf, inner, wide, rows, slots, total, hits, w_sem, z_send, z_recv, in_send, in_recv, slot_send, slot_recv, ring_send, ring_recv, pair_send, pair_recv):
    me = lax.axis_index("sp")
    core = me % 2
    chip = me // 2
    chips = group // 2
    other = me + 1 - 2 * core
    ahead = (me + 2 - 4 * core + group) % group
    depth = wbuf.shape[0]
    part = wbuf.shape[2]
    half_in, half_out = b1_ref.shape[0] // 2, b2_ref.shape[0] // 2
    count = half_in + half_out
    merged_dev, merge_dim = patch_ref.shape
    vit = lnw_ref.shape[1]

    def weight_copy(j):
        slot = j % depth
        w_ref, index = (w1_ref, core * half_in + j) if j < half_in else (w2_ref, core * half_out + j - half_in)
        cols = pl.ds(pl.multiple_of(index * part, part), part)
        return pltpu.make_async_copy(w_ref.at[:, cols], wbuf.at[slot], w_sem.at[slot])

    for j in range(depth - 1):
        weight_copy(j).start()
    for n in range(merge_dim // vit):
        seg = slice(n * vit, (n + 1) * vit)
        z[core, :, seg] = layer_norm(patch_ref[:, seg], lnw_ref[...], lnb_ref[...])
    total[...] = jnp.zeros_like(total)
    hits[...] = jnp.zeros_like(hits)
    slots[me] = slots_ref[...]
    greet_group(group, me)

    def to_other(src, dst, send_sem, recv_sem):
        return pltpu.make_async_remote_copy(src_ref=src, dst_ref=dst, send_sem=send_sem, recv_sem=recv_sem, device_id={"sp": other}, device_id_type=MESH)

    def arrive(ref, sem):
        pltpu.make_async_copy(ref, ref, sem).wait()

    def slot_copy(k):
        return pltpu.make_async_remote_copy(
            src_ref=slots_ref, dst_ref=slots.at[me], send_sem=slot_send.at[k], recv_sem=slot_recv.at[me],
            device_id={"sp": lax.rem(me + k, group)}, device_id_type=MESH,
        )

    z_copy = to_other(z.at[core], z.at[core], z_send, z_recv)
    z_copy.start()
    for k in range(1, group):
        slot_copy(k).start()
    arrive(z.at[1 - core], z_recv)

    def inner_copy(j):
        mine = inner.at[core * half_in + j]
        return to_other(mine, mine, in_send.at[j], in_recv.at[j])

    def origin(lane, step):
        return (chip - (1 - 2 * lane) * step + chips) % chips

    def ring_copy(step, piece):
        held = rows.at[core, origin(core, step), piece]
        return pltpu.make_async_remote_copy(
            src_ref=held, dst_ref=held, send_sem=ring_send.at[step, piece], recv_sem=ring_recv.at[step, piece],
            device_id={"sp": ahead}, device_id_type=MESH,
        )

    def pair_copy(step, piece):
        held = rows.at[core, origin(core, step), piece]
        return to_other(held, held, pair_send.at[step, piece], pair_recv.at[step, piece])

    for j in range(half_in):
        weight_copy(j + depth - 1).start()
        weight_copy(j).wait()
        lin = jnp.dot(z[...].reshape(2 * merged_dev, merge_dim), wbuf[j % depth], preferred_element_type=jnp.float32)
        lin = lin + b1_ref[core * half_in + j].astype(jnp.float32)
        inner[core * half_in + j] = (lin * (0.5 * (1.0 + lax.erf(lin * 0.7071067811865476)))).astype(jnp.bfloat16)
        if j > 0:
            inner_copy(j - 1).start()
    inner_copy(half_in - 1).start()
    for j in range(half_in):
        arrive(inner.at[(1 - core) * half_in + j], in_recv.at[j])
    for j in range(2 * half_in):
        wide[:, j * part:(j + 1) * part] = inner[j]
    for j in range(half_in, count):
        piece = j - half_in
        if j + depth - 1 < count:
            weight_copy(j + depth - 1).start()
        weight_copy(j).wait()
        lin = jnp.dot(wide[...], wbuf[j % depth], preferred_element_type=jnp.float32)
        rows[core, chip, piece] = (lin + b2_ref[core * half_out + piece].astype(jnp.float32)).astype(jnp.bfloat16)
        if piece > 0:
            ring_copy(0, piece - 1).start()
            pair_copy(0, piece - 1).start()
    tokens = embeds_ref.shape[0]
    wanted = me * tokens + lax.broadcasted_iota(jnp.int32, (tokens, 1), 0)
    for k in range(1, group):
        dev = lax.rem(me + k, group)
        arrive(slots.at[dev], slot_recv.at[dev])
    ring_copy(0, half_out - 1).start()
    pair_copy(0, half_out - 1).start()

    def choose(block):
        return jnp.concatenate([jnp.where(slots[2 * block + n] == wanted, 1.0, 0.0) for n in range(2)], axis=1)

    def place(lane, block, pick):
        for piece in range(half_out):
            total[lane * half_out + piece] += jnp.dot(pick, rows[lane, block, piece], preferred_element_type=jnp.float32)

    def hop(step, carry):
        mine, theirs = origin(core, step), origin(1 - core, step)

        @pl.when(step > 0)
        def _():
            for piece in range(half_out):
                arrive(rows.at[core, mine, piece], ring_recv.at[(step + chips - 1) % chips, piece])

                @pl.when(step < chips - 1)
                def _():
                    ring_copy(step, piece).start()

                pair_copy(step, piece).start()

        pick = choose(mine)
        hits[...] += pick
        place(core, mine, pick.astype(jnp.bfloat16))
        for piece in range(half_out):
            arrive(rows.at[1 - core, theirs, piece], pair_recv.at[step, piece])
        place(1 - core, theirs, choose(theirs).astype(jnp.bfloat16))
        return carry

    lax.fori_loop(0, chips, hop, 0)
    found = jnp.max(hits[...], axis=1, keepdims=True) > 0.0
    for n in range(2 * half_out):
        cols = slice(n * part, (n + 1) * part)
        h_ref[:, cols] = jnp.where(found, total[n].astype(jnp.bfloat16), embeds_ref[:, cols])
    a_ref[...] = rms_norm(h_ref[...], gain_ref[...])
    z_copy.wait_send()
    for k in range(1, group):
        slot_copy(k).wait_send()
    for j in range(half_in):
        inner_copy(j).wait_send()

    def drain(step, carry):
        for piece in range(half_out):
            @pl.when(step < chips - 1)
            def _():
                ring_copy(step, piece).wait_send()

            pair_copy(step, piece).wait_send()
        return carry

    lax.fori_loop(0, chips, drain, 0)


def merge_place(group, patches, ln_w, ln_b, w_one, b_one, w_two, b_two, dest_slot, embeds, gain):
    merged_dev = dest_slot.shape[0]
    merge_dim, width = w_two.shape
    tokens = embeds.shape[0]
    vit = ln_w.shape[0]
    part = 2 * HEAD_DIM
    chips = group // 2
    n_in, n_out = merge_dim // part, width // part
    vmem = pl.BlockSpec(memory_space=pltpu.VMEM)
    hbm = pl.BlockSpec(memory_space=pl.ANY)
    out = jax.ShapeDtypeStruct((tokens, width), jnp.bfloat16)
    ring = pltpu.SemaphoreType.DMA((chips, n_out // 2))
    return pl.pallas_call(
        functools.partial(merge_place_kernel, group),
        out_shape=(out, out),
        in_specs=[vmem] * 8 + [hbm, hbm],
        out_specs=(vmem, vmem),
        scratch_shapes=[
            pltpu.VMEM((2, merged_dev, merge_dim), jnp.bfloat16),
            pltpu.VMEM((3, merge_dim, part), jnp.bfloat16),
            pltpu.VMEM((n_in, 2 * merged_dev, part), jnp.bfloat16),
            pltpu.VMEM((2 * merged_dev, merge_dim), jnp.bfloat16),
            pltpu.VMEM((2, chips, n_out // 2, 2 * merged_dev, part), jnp.bfloat16),
            pltpu.VMEM((group, 1, merged_dev), jnp.int32),
            pltpu.VMEM((n_out, tokens, part), jnp.float32),
            pltpu.VMEM((tokens, 2 * merged_dev), jnp.float32),
            pltpu.SemaphoreType.DMA((3,)),
            pltpu.SemaphoreType.DMA,
            pltpu.SemaphoreType.DMA,
            pltpu.SemaphoreType.DMA((n_in // 2,)),
            pltpu.SemaphoreType.DMA((n_in // 2,)),
            pltpu.SemaphoreType.DMA((group,)),
            pltpu.SemaphoreType.DMA((group,)),
            ring,
            ring,
            ring,
            ring,
        ],
        compiler_params=pltpu.CompilerParams(collective_id=2, has_side_effects=True, vmem_limit_bytes=VMEM_LIMIT),
        cost_estimate=pl.CostEstimate(flops=2 * merged_dev * merge_dim * (merge_dim + width), bytes_accessed=merge_dim * (merge_dim + width), transcendentals=0),
        name="merge_place",
    )(
        patches.reshape(merged_dev, merge_dim), ln_w.reshape(1, vit), ln_b.reshape(1, vit), b_one.reshape(n_in, 1, part), b_two.reshape(n_out, 1, part),
        dest_slot.reshape(1, merged_dev), embeds, gain.reshape(1, width), w_one, w_two,
    )


def mlp_kernel(o_cols, chunk, attn_ref, h_ref, gain_ref, wo_ref, wg_ref, wu_ref, wd_ref, out_ref, attn, h_one, normed, total, wo, wg, wu, wd, o_sem, f_sem):
    heads, _, dim = attn_ref.shape
    width = h_ref.shape[1]
    o_steps, steps = width // o_cols, wg_ref.shape[1] // chunk

    def o_copy(i):
        return pltpu.make_async_copy(wo_ref.at[:, pl.ds(i * o_cols, o_cols)], wo.at[i % 2], o_sem.at[i % 2])

    def f_copies(i):
        b = i % 2
        cols = pl.ds(pl.multiple_of(i * chunk, 128), chunk)
        return [
            pltpu.make_async_copy(wg_ref.at[:, cols], wg.at[b], f_sem.at[b, 0]),
            pltpu.make_async_copy(wu_ref.at[:, cols], wu.at[b], f_sem.at[b, 1]),
            pltpu.make_async_copy(wd_ref.at[cols, :], wd.at[b], f_sem.at[b, 2]),
        ]

    o_copy(0).start()
    o_copy(1).start()
    for h in range(heads):
        attn[:, h * dim:(h + 1) * dim] = attn_ref[h]
    for i in range(o_steps):
        o_copy(i).wait()
        cols = slice(i * o_cols, (i + 1) * o_cols)
        part = jnp.dot(attn[...], wo[i % 2], preferred_element_type=jnp.float32)
        h_one[:, cols] = (h_ref[:, cols].astype(jnp.float32) + part).astype(jnp.bfloat16)
        if i + 2 < o_steps:
            o_copy(i + 2).start()
        if i == o_steps - 3:
            for c in f_copies(0):
                c.start()
    normed[...] = rms_norm(h_one[...], gain_ref[...])
    total[...] = h_one[...].astype(jnp.float32)

    def step(i, carry):
        b = i % 2

        @pl.when(i + 1 < steps)
        def _():
            for c in f_copies(i + 1):
                c.start()

        gate_copy, up_copy, down_copy = f_copies(i)
        gate_copy.wait()
        up_copy.wait()
        gate_pre = jnp.dot(normed[...], wg[b], preferred_element_type=jnp.float32)
        up_pre = jnp.dot(normed[...], wu[b], preferred_element_type=jnp.float32)
        activated = (jax.nn.silu(gate_pre) * up_pre).astype(jnp.bfloat16)
        down_copy.wait()
        total[...] += jnp.dot(activated, wd[b], preferred_element_type=jnp.float32)
        return carry

    lax.fori_loop(0, steps, step, 0)
    out_ref[...] = total[...].astype(jnp.bfloat16)


def mlp(attn, h_zero, gain, w_o, w_gate, w_up, w_down):
    heads, tokens, dim = attn.shape
    width, ffn = w_gate.shape
    o_cols = width // 5
    chunk = ffn // 9
    vmem = pl.BlockSpec(memory_space=pltpu.VMEM)
    hbm = pl.BlockSpec(memory_space=pl.ANY)
    return pl.pallas_call(
        functools.partial(mlp_kernel, o_cols, chunk),
        out_shape=jax.ShapeDtypeStruct((tokens, width), jnp.bfloat16),
        in_specs=[vmem, vmem, vmem, hbm, hbm, hbm, hbm],
        out_specs=vmem,
        scratch_shapes=[
            pltpu.VMEM((tokens, heads * dim), jnp.bfloat16),
            pltpu.VMEM((tokens, width), jnp.bfloat16),
            pltpu.VMEM((tokens, width), jnp.bfloat16),
            pltpu.VMEM((tokens, width), jnp.float32),
            pltpu.VMEM((2, heads * dim, o_cols), jnp.bfloat16),
            pltpu.VMEM((2, width, chunk), jnp.bfloat16),
            pltpu.VMEM((2, width, chunk), jnp.bfloat16),
            pltpu.VMEM((2, chunk, width), jnp.bfloat16),
            pltpu.SemaphoreType.DMA((2,)),
            pltpu.SemaphoreType.DMA((2, 3)),
        ],
        compiler_params=pltpu.CompilerParams(vmem_limit_bytes=VMEM_LIMIT),
        cost_estimate=pl.CostEstimate(flops=2 * tokens * width * (3 * ffn + width), bytes_accessed=2 * width * (3 * ffn + width), transcendentals=tokens * ffn),
        name="mlp",
    )(attn, h_zero, gain.reshape(1, width), w_o, w_gate, w_up, w_down)


def solution(mesh):
    group = mesh.shape['sp']
    row_spec = P(('dp', 'sp'), None)

    def local_step(patches, embeds, dest_slot, rope_pos, cu_doc, ln_w, ln_b, w_one, b_one, w_two, b_two, norm_attn, w_q, b_q, w_k, b_k, w_v, b_v, w_o, norm_mlp, w_gate, w_up, w_down):
        heads = w_q.shape[1] // HEAD_DIM
        h_zero, normed_a = merge_place(group, patches, ln_w, ln_b, w_one, b_one, w_two, b_two, dest_slot, embeds, norm_attn)
        cos_t, sin_t = rope_tables(rope_pos)
        biases = jnp.concatenate([b.astype(jnp.float32).reshape(heads, 1, HEAD_DIM) for b in (b_q, b_k, b_v)], axis=2)
        attn_out = mixer(group, heads, cu_doc, normed_a, cos_t, sin_t, biases, w_q, w_k, w_v)
        return mlp(attn_out, h_zero, norm_mlp, w_o, w_gate, w_up, w_down)

    in_specs = (row_spec, row_spec, P(('dp', 'sp')), P(None, ('dp', 'sp')), P('dp')) + (P(),) * 18
    return jax.shard_map(local_step, mesh=mesh, in_specs=in_specs, out_specs=row_spec, check_vma=False)
```

```python
import functools

import jax
import jax.numpy as jnp
from jax import lax
from jax.experimental import pallas as pl
from jax.experimental.pallas import tpu as pltpu
from jax.sharding import PartitionSpec as P

HEAD_DIM = 128
NORM_EPS = 1e-6
ROPE_THETA = 1000000.0
MROPE_SPLIT = (16, 40)
MESH = pl.DeviceIdType.MESH
VMEM_LIMIT = 60 * 1024 * 1024
MIXER_VMEM = 42 * 1024 * 1024
MLP_VMEM = 46 * 1024 * 1024


def rms_norm(values_in, gain_vec):
    widened = values_in.astype(jnp.float32)
    return (widened * lax.rsqrt(jnp.mean(widened * widened, axis=-1, keepdims=True) + NORM_EPS) * gain_vec.astype(jnp.float32)).astype(jnp.bfloat16)


def rope_tables(rope_pos):
    inv_freq = ROPE_THETA ** (-jnp.arange(0, HEAD_DIM, 2, dtype=jnp.float32) / HEAD_DIM)
    freq_idx = jnp.arange(HEAD_DIM // 2)[None, :]
    chosen = jnp.where(freq_idx < MROPE_SPLIT[0], rope_pos[0][:, None], jnp.where(freq_idx < MROPE_SPLIT[1], rope_pos[1][:, None], rope_pos[2][:, None]))
    angles = chosen.astype(jnp.float32) * inv_freq[None, :]
    cos_h, sin_h = jnp.cos(angles), jnp.sin(angles)
    return jnp.concatenate([cos_h, cos_h], axis=-1), jnp.concatenate([-sin_h, sin_h], axis=-1)


def first_head(dev, group, heads):
    return (dev * heads + group - 1) // group


def owner_of(head, group, heads):
    return head * group // heads


def greet_group(group, me):
    barrier = pltpu.get_barrier_semaphore()
    for k in range(1, group):
        pl.semaphore_signal(barrier, inc=1, device_id={"sp": lax.rem(me + k, group)}, device_id_type=MESH)
    pl.semaphore_wait(barrier, group - 1)


def mixer_kernel(group, heads, cuts, bias_at, cu_ref, a_ref, cos_ref, sin_ref, vec_ref, wq_ref, wk_ref, wv_ref, attn_ref, wbuf, stage, land, top_ref, sum_ref, acc_ref, o_ref, w_sem, send_sem, recv_sem, own_sem, o_send, o_recv, o_own):
    me = lax.axis_index("sp")
    chips = group // 2
    my_chip = me // 2
    depth = wbuf.shape[0]
    slots = land.shape[0]
    tokens = a_ref.shape[0]
    rows = 2 * tokens
    mine = first_head(me, group, heads)
    count = first_head(me + 1, group, heads) - mine

    def head_at(p):
        step = (p + 1) // 2
        return (mine + (2 * (p % 2) - 1) * step + heads) % heads

    def weight_copies(p):
        cols = pl.ds(pl.multiple_of(head_at(p) * HEAD_DIM, HEAD_DIM), HEAD_DIM)
        slot = p % depth
        return [
            pltpu.make_async_copy(w.at[:, cols], wbuf.at[slot, :, pl.ds(n * HEAD_DIM, HEAD_DIM)], w_sem.at[slot, n])
            for n, w in enumerate((wq_ref, wk_ref, wv_ref))
        ]

    def remote(p):
        head = head_at(p)
        target = owner_of(head, group, heads)
        slot = head - first_head(target, group, heads)
        copy = pltpu.make_async_remote_copy(
            src_ref=stage.at[p],
            dst_ref=land.at[slot, me],
            send_sem=send_sem.at[p],
            recv_sem=recv_sem.at[slot, me],
            device_id={"sp": target},
            device_id_type=MESH,
        )
        local = pltpu.make_async_copy(stage.at[p], land.at[slot, me], own_sem.at[slot])
        return target, copy, local

    def send(p):
        target, copy, local = remote(p)

        @pl.when(target != me)
        def _():
            copy.start()

        @pl.when(target == me)
        def _():
            local.start()

    for p in range(depth - 1):
        for c in weight_copies(p):
            c.start()
    greet_group(group, me)

    def project(p, carry):
        @pl.when(p + depth - 1 < heads)
        def _():
            for c in weight_copies(p + depth - 1):
                c.start()

        for c in weight_copies(p):
            c.wait()
        lin = jnp.dot(a_ref[...], wbuf[p % depth], preferred_element_type=jnp.float32)
        lin = lin + jnp.concatenate([vec_ref[:, pl.ds(pl.multiple_of(at + head_at(p) * HEAD_DIM, HEAD_DIM), HEAD_DIM)] for at in bias_at], axis=1)

        @pl.when(p > 0)
        def _():
            send(p - 1)

        cos_t, sin_t = cos_ref[...], sin_ref[...]
        for n in range(3):
            part = lin[:, n * HEAD_DIM:(n + 1) * HEAD_DIM]
            if n < 2:
                part = part * cos_t + pltpu.roll(part, HEAD_DIM // 2, 1) * sin_t
            stage[p, n] = part.astype(jnp.bfloat16)
        return carry

    lax.fori_loop(0, heads, project, 0)

    def clear(c, carry):
        for slot in range(slots):
            top_ref[slot, c] = jnp.full((rows, HEAD_DIM), -1e30, jnp.float32)
            sum_ref[slot, c] = jnp.zeros((rows, HEAD_DIM), jnp.float32)
            acc_ref[slot, c] = jnp.zeros((rows, HEAD_DIM), jnp.float32)
        return carry

    send(heads - 1)
    lax.fori_loop(0, chips, clear, 0)
    scale = HEAD_DIM ** -0.5 * 1.4426950408889634

    def chip_at(t):
        step = (t + 1) // 2
        return (my_chip + (2 * (t % 2) - 1) * step + chips) % chips

    def block(slot, part, chip):
        return land[slot, pl.ds(2 * chip, 2), part].reshape(rows, HEAD_DIM)

    def attend(slot, q_chip, k_chip, causal):
        scores = lax.dot_general(block(slot, 0, q_chip), block(slot, 1, k_chip), (((1,), (1,)), ((), ())), preferred_element_type=jnp.float32)
        q_pos = q_chip * rows + lax.broadcasted_iota(jnp.int32, (rows, 1), 0)
        q_low = jnp.zeros((rows, 1), jnp.int32)
        for d in range(1, cuts + 1):
            q_low = jnp.where(q_pos >= cu_ref[d], cu_ref[d], q_low)
        k_pos = k_chip * rows + lax.broadcasted_iota(jnp.int32, (1, rows), 1)
        seen = k_pos >= q_low
        if causal:
            seen = seen & (k_pos <= q_pos)
        scores = jnp.where(seen, scores, -1e30)
        top = top_ref[slot, q_chip]
        new_top = jnp.maximum(top, jnp.max(scores, axis=1, keepdims=True))
        decay = jnp.exp2((top - new_top) * scale)
        total = sum_ref[slot, q_chip] * decay
        parts = []
        for n in range(rows // HEAD_DIM):
            probs = jnp.exp2((scores[:, n * HEAD_DIM:(n + 1) * HEAD_DIM] - new_top) * scale)
            total = total + probs
            parts.append(probs.astype(jnp.bfloat16))
        mixed = jnp.dot(jnp.concatenate(parts, axis=1), block(slot, 2, k_chip), preferred_element_type=jnp.float32)
        top_ref[slot, q_chip] = new_top
        sum_ref[slot, q_chip] = total
        acc_ref[slot, q_chip] = acc_ref[slot, q_chip] * decay + mixed

    def for_slots(action):
        lax.fori_loop(0, count, lambda slot, carry: (action(slot), carry)[1], 0)

    def wait_chip(chip):
        def one(slot):
            for core in range(2):
                dev = 2 * chip + core
                landed = land.at[slot, dev]

                @pl.when(dev != me)
                def _():
                    pltpu.make_async_copy(landed, landed, recv_sem.at[slot, dev]).wait()

                @pl.when(dev == me)
                def _():
                    pltpu.make_async_copy(landed, landed, own_sem.at[slot]).wait()

        for_slots(one)

    def pair(t, u):
        here, there = chip_at(t), chip_at(u)
        later = (here - there + chips) // chips
        q_chip = here * later + there * (1 - later)
        k_chip = there * later + here * (1 - later)
        for_slots(lambda slot: attend(slot, q_chip, k_chip, False))

    def o_copy(slot, dev):
        return pltpu.make_async_remote_copy(
            src_ref=o_ref.at[slot, dev],
            dst_ref=attn_ref.at[mine + slot],
            send_sem=o_send.at[slot, dev],
            recv_sem=o_recv.at[mine + slot],
            device_id={"sp": dev},
            device_id_type=MESH,
        )

    def o_local(slot):
        return pltpu.make_async_copy(o_ref.at[slot, me], attn_ref.at[mine + slot], o_own.at[slot])

    def finish(chip):
        def divide(slot):
            total = jnp.sum(sum_ref[slot, chip], axis=1, keepdims=True)
            out = (acc_ref[slot, chip] / total).astype(jnp.bfloat16)
            o_ref[slot, pl.ds(2 * chip, 2)] = out.reshape(2, tokens, HEAD_DIM)

        def give(slot):
            for core in range(2):
                dev = 2 * chip + core

                @pl.when(dev != me)
                def _():
                    o_copy(slot, dev).start()

                @pl.when(dev == me)
                def _():
                    o_local(slot).start()

        for_slots(divide)
        for_slots(give)

    def arrival(t, carry):
        chip = chip_at(t)
        wait_chip(chip)
        for_slots(lambda slot: attend(slot, chip, chip, True))
        lax.fori_loop(0, t, lambda u, c: (pair(t, u), c)[1], 0)
        return carry

    last = chips - 1
    far = chip_at(last)
    lax.fori_loop(0, last, arrival, 0)

    def early(u, carry):
        @pl.when(chip_at(u) < far)
        def _():
            finish(chip_at(u))

        return carry

    lax.fori_loop(0, last, early, 0)
    wait_chip(far)
    for_slots(lambda slot: attend(slot, far, far, True))

    def late(u, carry):
        pair(last, u)

        @pl.when(chip_at(u) > far)
        def _():
            finish(chip_at(u))

        return carry

    lax.fori_loop(0, last, late, 0)
    finish(far)

    def drain(p, carry):
        target, copy, _ = remote(p)

        @pl.when(target != me)
        def _():
            copy.wait_send()

        return carry

    lax.fori_loop(0, heads, drain, 0)

    def drain_out(slot):
        def one(dev, carry):
            @pl.when(dev != me)
            def _():
                o_copy(slot, dev).wait_send()

            return carry

        lax.fori_loop(0, group, one, 0)
        o_local(slot).wait()

    for_slots(drain_out)

    def landed_out(head, carry):
        @pl.when(owner_of(head, group, heads) != me)
        def _():
            back = attn_ref.at[head]
            pltpu.make_async_copy(back, back, o_recv.at[head]).wait()

        return carry

    lax.fori_loop(0, heads, landed_out, 0)


def mixer(group, heads, cu_doc, normed, cos_t, sin_t, vectors, bias_at, w_q, w_k, w_v):
    tokens, width = normed.shape
    slots = -(-heads // group)
    chips = group // 2
    vmem = pl.BlockSpec(memory_space=pltpu.VMEM)
    smem = pl.BlockSpec(memory_space=pltpu.SMEM)
    hbm = pl.BlockSpec(memory_space=pl.ANY)
    state = pltpu.VMEM((slots, chips, 2 * tokens, HEAD_DIM), jnp.float32)
    return pl.pallas_call(
        functools.partial(mixer_kernel, group, heads, cu_doc.shape[0] - 2, bias_at),
        out_shape=jax.ShapeDtypeStruct((heads, tokens, HEAD_DIM), jnp.bfloat16),
        in_specs=[smem, vmem, vmem, vmem, vmem, hbm, hbm, hbm],
        out_specs=hbm,
        scratch_shapes=[
            pltpu.VMEM((3, width, 3 * HEAD_DIM), jnp.bfloat16),
            pltpu.VMEM((heads, 3, tokens, HEAD_DIM), jnp.bfloat16),
            pltpu.VMEM((slots, group, 3, tokens, HEAD_DIM), jnp.bfloat16),
            state,
            state,
            state,
            pltpu.VMEM((slots, group, tokens, HEAD_DIM), jnp.bfloat16),
            pltpu.SemaphoreType.DMA((3, 3)),
            pltpu.SemaphoreType.DMA((heads,)),
            pltpu.SemaphoreType.DMA((slots, group)),
            pltpu.SemaphoreType.DMA((slots,)),
            pltpu.SemaphoreType.DMA((slots, group)),
            pltpu.SemaphoreType.DMA((heads,)),
            pltpu.SemaphoreType.DMA((slots,)),
        ],
        compiler_params=pltpu.CompilerParams(collective_id=0, has_side_effects=True, vmem_limit_bytes=MIXER_VMEM),
        cost_estimate=pl.CostEstimate(flops=2 * tokens * width * 3 * heads * HEAD_DIM, bytes_accessed=3 * width * heads * HEAD_DIM * 2, transcendentals=0),
        name="mixer",
    )(cu_doc, normed, cos_t, sin_t, vectors, w_q, w_k, w_v)


def merge_place_kernel(group, patch_ref, vec_ref, slots_ref, embeds_ref, w1_ref, w2_ref, h_ref, a_ref, z, scaled, wbuf, inner, wide, rows, slots, total, hits, w_sem, z_send, z_recv, in_send, in_recv, slot_send, slot_recv, ring_send, ring_recv, pair_send, pair_recv):
    me = lax.axis_index("sp")
    core = me % 2
    chip = me // 2
    chips = group // 2
    other = me + 1 - 2 * core
    ahead = (me + 2 - 4 * core + group) % group
    depth = wbuf.shape[0]
    part = wbuf.shape[2]
    merged_dev, vit = slots_ref.shape[1], patch_ref.shape[1]
    merge_dim, width = w2_ref.shape
    half_in, half_out = merge_dim // (2 * part), width // (2 * part)
    count = half_in + half_out
    after = [0]
    for size in (vit, vit, merge_dim, width, width):
        after.append(after[-1] + size)

    def vector(n):
        return vec_ref[:, after[n]:after[n + 1]]

    def bias(n, index):
        return vec_ref[:, pl.ds(pl.multiple_of(after[n] + index * part, HEAD_DIM), part)]

    def weight_copy(j):
        slot = j % depth
        w_ref, index = (w1_ref, core * half_in + j) if j < half_in else (w2_ref, core * half_out + j - half_in)
        cols = pl.ds(pl.multiple_of(index * part, part), part)
        return pltpu.make_async_copy(w_ref.at[:, cols], wbuf.at[slot], w_sem.at[slot])

    for j in range(depth - 1):
        weight_copy(j).start()
    widened = patch_ref[...].astype(jnp.float32)
    centered = widened - jnp.mean(widened, axis=-1, keepdims=True)
    spread = jnp.mean(centered * centered, axis=-1, keepdims=True)
    normed = centered * lax.rsqrt(spread + NORM_EPS) * vector(0) + vector(1)
    for c in range(vit // HEAD_DIM):
        scaled[c] = normed[:, c * HEAD_DIM:(c + 1) * HEAD_DIM]
    merge = merge_dim // vit
    for n in range(merge):
        for c in range(vit // HEAD_DIM):
            lanes = n * vit + c * HEAD_DIM
            z[core, :, lanes:lanes + HEAD_DIM] = scaled[c, pl.ds(n, merged_dev, stride=merge), :].astype(jnp.bfloat16)
    total[...] = jnp.zeros_like(total)
    hits[...] = jnp.zeros_like(hits)
    slots[me] = slots_ref[...]
    greet_group(group, me)

    def to_other(src, dst, send_sem, recv_sem):
        return pltpu.make_async_remote_copy(src_ref=src, dst_ref=dst, send_sem=send_sem, recv_sem=recv_sem, device_id={"sp": other}, device_id_type=MESH)

    def arrive(ref, sem):
        pltpu.make_async_copy(ref, ref, sem).wait()

    def slot_copy(k):
        return pltpu.make_async_remote_copy(
            src_ref=slots_ref, dst_ref=slots.at[me], send_sem=slot_send.at[k], recv_sem=slot_recv.at[me],
            device_id={"sp": lax.rem(me + k, group)}, device_id_type=MESH,
        )

    z_copy = to_other(z.at[core], z.at[core], z_send, z_recv)
    z_copy.start()
    for k in range(1, group):
        slot_copy(k).start()
    arrive(z.at[1 - core], z_recv)

    def inner_copy(j):
        mine = inner.at[core * half_in + j]
        return to_other(mine, mine, in_send.at[j], in_recv.at[j])

    def origin(lane, step):
        return (chip - (1 - 2 * lane) * step + chips) % chips

    def ring_copy(step, piece):
        held = rows.at[core, origin(core, step), piece]
        return pltpu.make_async_remote_copy(
            src_ref=held, dst_ref=held, send_sem=ring_send.at[step, piece], recv_sem=ring_recv.at[step, piece],
            device_id={"sp": ahead}, device_id_type=MESH,
        )

    def pair_copy(step, piece):
        held = rows.at[core, origin(core, step), piece]
        return to_other(held, held, pair_send.at[step, piece], pair_recv.at[step, piece])

    for j in range(half_in):
        weight_copy(j + depth - 1).start()
        weight_copy(j).wait()
        lin = jnp.dot(z[...].reshape(2 * merged_dev, merge_dim), wbuf[j % depth], preferred_element_type=jnp.float32)
        lin = lin + bias(2, core * half_in + j)
        inner[core * half_in + j] = (lin * (0.5 * (1.0 + lax.erf(lin * 0.7071067811865476)))).astype(jnp.bfloat16)
        if j > 0:
            inner_copy(j - 1).start()
    inner_copy(half_in - 1).start()
    for j in range(half_in):
        arrive(inner.at[(1 - core) * half_in + j], in_recv.at[j])
    for j in range(2 * half_in):
        wide[:, j * part:(j + 1) * part] = inner[j]
    for j in range(half_in, count):
        piece = j - half_in
        if j + depth - 1 < count:
            weight_copy(j + depth - 1).start()
        weight_copy(j).wait()
        lin = jnp.dot(wide[...], wbuf[j % depth], preferred_element_type=jnp.float32)
        rows[core, chip, piece] = (lin + bias(3, core * half_out + piece)).astype(jnp.bfloat16)
        if piece > 0:
            ring_copy(0, piece - 1).start()
            pair_copy(0, piece - 1).start()
    tokens = embeds_ref.shape[0]
    wanted = me * tokens + lax.broadcasted_iota(jnp.int32, (tokens, 1), 0)
    for k in range(1, group):
        dev = lax.rem(me + k, group)
        arrive(slots.at[dev], slot_recv.at[dev])
    ring_copy(0, half_out - 1).start()
    pair_copy(0, half_out - 1).start()

    def choose(block):
        return jnp.concatenate([jnp.where(slots[2 * block + n] == wanted, 1.0, 0.0) for n in range(2)], axis=1)

    def place(lane, block, piece, pick):
        total[lane * half_out + piece] += jnp.dot(pick, rows[lane, block, piece], preferred_element_type=jnp.float32)

    def hop(step, carry):
        mine, theirs = origin(core, step - 1), origin(1 - core, step - 1)
        pick, pick_theirs = choose(mine), choose(theirs).astype(jnp.bfloat16)
        hits[...] += pick
        pick = pick.astype(jnp.bfloat16)
        for piece in range(half_out):

            @pl.when(step < chips)
            def _():
                arrive(rows.at[core, origin(core, step), piece], ring_recv.at[step - 1, piece])

                @pl.when(step < chips - 1)
                def _():
                    ring_copy(step, piece).start()

                pair_copy(step, piece).start()

            place(core, mine, piece, pick)
            arrive(rows.at[1 - core, theirs, piece], pair_recv.at[step - 1, piece])
            place(1 - core, theirs, piece, pick_theirs)
        return carry

    lax.fori_loop(1, chips + 1, hop, 0)
    found = jnp.max(hits[...], axis=1, keepdims=True) > 0.0
    for n in range(2 * half_out):
        cols = slice(n * part, (n + 1) * part)
        h_ref[:, cols] = jnp.where(found, total[n].astype(jnp.bfloat16), embeds_ref[:, cols])
    a_ref[...] = rms_norm(h_ref[...], vector(4))
    z_copy.wait_send()
    for k in range(1, group):
        slot_copy(k).wait_send()
    for j in range(half_in):
        inner_copy(j).wait_send()

    def drain(step, carry):
        for piece in range(half_out):
            @pl.when(step < chips - 1)
            def _():
                ring_copy(step, piece).wait_send()

            pair_copy(step, piece).wait_send()
        return carry

    lax.fori_loop(0, chips, drain, 0)


def merge_place(group, patches, vectors, w_one, w_two, dest_slot, embeds):
    merged_dev = dest_slot.shape[0]
    merge_dim, width = w_two.shape
    tokens = embeds.shape[0]
    part = 2 * HEAD_DIM
    chips = group // 2
    n_in, n_out = merge_dim // part, width // part
    vmem = pl.BlockSpec(memory_space=pltpu.VMEM)
    hbm = pl.BlockSpec(memory_space=pl.ANY)
    out = jax.ShapeDtypeStruct((tokens, width), jnp.bfloat16)
    ring = pltpu.SemaphoreType.DMA((chips, n_out // 2))
    return pl.pallas_call(
        functools.partial(merge_place_kernel, group),
        out_shape=(out, out),
        in_specs=[vmem] * 4 + [hbm, hbm],
        out_specs=(vmem, vmem),
        scratch_shapes=[
            pltpu.VMEM((2, merged_dev, merge_dim), jnp.bfloat16),
            pltpu.VMEM((patches.shape[1] // HEAD_DIM, patches.shape[0], HEAD_DIM), jnp.float32),
            pltpu.VMEM((3, merge_dim, part), jnp.bfloat16),
            pltpu.VMEM((n_in, 2 * merged_dev, part), jnp.bfloat16),
            pltpu.VMEM((2 * merged_dev, merge_dim), jnp.bfloat16),
            pltpu.VMEM((2, chips, n_out // 2, 2 * merged_dev, part), jnp.bfloat16),
            pltpu.VMEM((group, 1, merged_dev), jnp.int32),
            pltpu.VMEM((n_out, tokens, part), jnp.float32),
            pltpu.VMEM((tokens, 2 * merged_dev), jnp.float32),
            pltpu.SemaphoreType.DMA((3,)),
            pltpu.SemaphoreType.DMA,
            pltpu.SemaphoreType.DMA,
            pltpu.SemaphoreType.DMA((n_in // 2,)),
            pltpu.SemaphoreType.DMA((n_in // 2,)),
            pltpu.SemaphoreType.DMA((group,)),
            pltpu.SemaphoreType.DMA((group,)),
            ring,
            ring,
            ring,
            ring,
        ],
        compiler_params=pltpu.CompilerParams(collective_id=2, has_side_effects=True, vmem_limit_bytes=VMEM_LIMIT),
        cost_estimate=pl.CostEstimate(flops=2 * merged_dev * merge_dim * (merge_dim + width), bytes_accessed=merge_dim * (merge_dim + width), transcendentals=0),
        name="merge_place",
    )(
        patches, vectors,
        dest_slot.reshape(1, merged_dev), embeds, w_one, w_two,
    )


def mlp_kernel(o_cols, chunk, gain_at, attn_ref, h_ref, vec_ref, wo_ref, wg_ref, wu_ref, wd_ref, out_ref, attn, h_one, normed, total, wo, wg, wu, wd, o_sem, f_sem):
    heads, _, dim = attn_ref.shape
    width = h_ref.shape[1]
    o_steps, steps = width // o_cols, wg_ref.shape[1] // chunk

    def o_copy(i):
        return pltpu.make_async_copy(wo_ref.at[:, pl.ds(i * o_cols, o_cols)], wo.at[i % 2], o_sem.at[i % 2])

    def f_copies(i):
        b = i % 2
        cols = pl.ds(pl.multiple_of(i * chunk, 128), chunk)
        return [
            pltpu.make_async_copy(wg_ref.at[:, cols], wg.at[b], f_sem.at[b, 0]),
            pltpu.make_async_copy(wu_ref.at[:, cols], wu.at[b], f_sem.at[b, 1]),
            pltpu.make_async_copy(wd_ref.at[cols, :], wd.at[b], f_sem.at[b, 2]),
        ]

    o_copy(0).start()
    o_copy(1).start()
    for h in range(heads):
        attn[:, h * dim:(h + 1) * dim] = attn_ref[h]
    for i in range(o_steps):
        o_copy(i).wait()
        cols = slice(i * o_cols, (i + 1) * o_cols)
        part = jnp.dot(attn[...], wo[i % 2], preferred_element_type=jnp.float32)
        h_one[:, cols] = (h_ref[:, cols].astype(jnp.float32) + part).astype(jnp.bfloat16)
        if i + 2 < o_steps:
            o_copy(i + 2).start()
        if i == o_steps - 3:
            for c in f_copies(0):
                c.start()
    normed[...] = rms_norm(h_one[...], vec_ref[:, gain_at:gain_at + width])
    total[...] = h_one[...].astype(jnp.float32)

    def step(i, carry):
        b = i % 2

        @pl.when(i + 1 < steps)
        def _():
            for c in f_copies(i + 1):
                c.start()

        gate_copy, up_copy, down_copy = f_copies(i)
        gate_copy.wait()
        up_copy.wait()
        gate_pre = jnp.dot(normed[...], wg[b], preferred_element_type=jnp.float32)
        up_pre = jnp.dot(normed[...], wu[b], preferred_element_type=jnp.float32)
        activated = (jax.nn.silu(gate_pre) * up_pre).astype(jnp.bfloat16)
        down_copy.wait()
        total[...] += jnp.dot(activated, wd[b], preferred_element_type=jnp.float32)
        return carry

    lax.fori_loop(0, steps, step, 0)
    out_ref[...] = total[...].astype(jnp.bfloat16)


def mlp(attn, h_zero, vectors, gain_at, w_o, w_gate, w_up, w_down):
    heads, tokens, dim = attn.shape
    width, ffn = w_gate.shape
    o_cols = width // 5
    chunk = ffn // 9
    vmem = pl.BlockSpec(memory_space=pltpu.VMEM)
    hbm = pl.BlockSpec(memory_space=pl.ANY)
    return pl.pallas_call(
        functools.partial(mlp_kernel, o_cols, chunk, gain_at),
        out_shape=jax.ShapeDtypeStruct((tokens, width), jnp.bfloat16),
        in_specs=[vmem, vmem, vmem, hbm, hbm, hbm, hbm],
        out_specs=vmem,
        scratch_shapes=[
            pltpu.VMEM((tokens, heads * dim), jnp.bfloat16),
            pltpu.VMEM((tokens, width), jnp.bfloat16),
            pltpu.VMEM((tokens, width), jnp.bfloat16),
            pltpu.VMEM((tokens, width), jnp.float32),
            pltpu.VMEM((2, heads * dim, o_cols), jnp.bfloat16),
            pltpu.VMEM((2, width, chunk), jnp.bfloat16),
            pltpu.VMEM((2, width, chunk), jnp.bfloat16),
            pltpu.VMEM((2, chunk, width), jnp.bfloat16),
            pltpu.SemaphoreType.DMA((2,)),
            pltpu.SemaphoreType.DMA((2, 3)),
        ],
        compiler_params=pltpu.CompilerParams(vmem_limit_bytes=MLP_VMEM),
        cost_estimate=pl.CostEstimate(flops=2 * tokens * width * (3 * ffn + width), bytes_accessed=2 * width * (3 * ffn + width), transcendentals=tokens * ffn),
        name="mlp",
    )(attn, h_zero, vectors, w_o, w_gate, w_up, w_down)


def solution(mesh):
    group = mesh.shape['sp']
    row_spec = P(('dp', 'sp'), None)

    def local_step(patches, embeds, dest_slot, rope_pos, cu_doc, ln_w, ln_b, w_one, b_one, w_two, b_two, norm_attn, w_q, b_q, w_k, b_k, w_v, b_v, w_o, norm_mlp, w_gate, w_up, w_down):
        heads = w_q.shape[1] // HEAD_DIM
        parts = (ln_w, ln_b, b_one, b_two, norm_attn, b_q, b_k, b_v, norm_mlp)
        starts = [sum(v.shape[0] for v in parts[:n]) for n in range(len(parts))]
        vectors = jnp.concatenate([v.astype(jnp.float32) for v in parts]).reshape(1, -1)
        cos_t, sin_t = rope_tables(rope_pos)
        h_zero, normed_a = merge_place(group, patches, vectors, w_one, w_two, dest_slot, embeds)
        attn_out = mixer(group, heads, cu_doc, normed_a, cos_t, sin_t, vectors, tuple(starts[5:8]), w_q, w_k, w_v)
        return mlp(attn_out, h_zero, vectors, starts[8], w_o, w_gate, w_up, w_down)

    in_specs = (row_spec, row_spec, P(('dp', 'sp')), P(None, ('dp', 'sp')), P('dp')) + (P(),) * 18
    return jax.shard_map(local_step, mesh=mesh, in_specs=in_specs, out_specs=row_spec, check_vma=False)
```

```python
import functools

import jax
import jax.numpy as jnp
from jax import lax
from jax.experimental import pallas as pl
from jax.experimental.pallas import tpu as pltpu
from jax.sharding import PartitionSpec as P

HEAD_DIM = 128
NORM_EPS = 1e-6
ROPE_THETA = 1000000.0
MROPE_SPLIT = (16, 40)
MESH = pl.DeviceIdType.MESH
VMEM_LIMIT = 60 * 1024 * 1024
MIXER_VMEM = 42 * 1024 * 1024
MLP_VMEM = 46 * 1024 * 1024


def rms_norm(values_in, gain_vec):
    widened = values_in.astype(jnp.float32)
    return (widened * lax.rsqrt(jnp.mean(widened * widened, axis=-1, keepdims=True) + NORM_EPS) * gain_vec.astype(jnp.float32)).astype(jnp.bfloat16)


def rope_tables(rope_pos):
    inv_freq = ROPE_THETA ** (-jnp.arange(0, HEAD_DIM, 2, dtype=jnp.float32) / HEAD_DIM)
    freq_idx = jnp.arange(HEAD_DIM // 2)[None, :]
    chosen = jnp.where(freq_idx < MROPE_SPLIT[0], rope_pos[0][:, None], jnp.where(freq_idx < MROPE_SPLIT[1], rope_pos[1][:, None], rope_pos[2][:, None]))
    angles = chosen.astype(jnp.float32) * inv_freq[None, :]
    cos_h, sin_h = jnp.cos(angles), jnp.sin(angles)
    return jnp.concatenate([cos_h, cos_h], axis=-1), jnp.concatenate([-sin_h, sin_h], axis=-1)


def first_head(dev, group, heads):
    return (dev * heads + group - 1) // group


def owner_of(head, group, heads):
    return head * group // heads


def greet_group(group, me):
    barrier = pltpu.get_barrier_semaphore()
    for k in range(1, group):
        pl.semaphore_signal(barrier, inc=1, device_id={"sp": lax.rem(me + k, group)}, device_id_type=MESH)
    pl.semaphore_wait(barrier, group - 1)


def mixer_kernel(group, heads, cuts, bias_at, cu_ref, a_ref, cos_ref, sin_ref, vec_ref, wq_ref, wk_ref, wv_ref, attn_ref, wbuf, stage, land, top_ref, sum_ref, acc_ref, o_ref, w_sem, send_sem, recv_sem, own_sem, o_send, o_recv, o_own):
    me = lax.axis_index("sp")
    chips = group // 2
    my_chip = me // 2
    depth = wbuf.shape[0]
    slots = land.shape[0]
    tokens = a_ref.shape[0]
    rows = 2 * tokens
    mine = first_head(me, group, heads)
    count = first_head(me + 1, group, heads) - mine

    def head_at(p):
        step = (p + 1) // 2
        return (mine + (2 * (p % 2) - 1) * step + heads) % heads

    def weight_copies(p):
        cols = pl.ds(pl.multiple_of(head_at(p) * HEAD_DIM, HEAD_DIM), HEAD_DIM)
        slot = p % depth
        return [
            pltpu.make_async_copy(w.at[:, cols], wbuf.at[slot, :, pl.ds(n * HEAD_DIM, HEAD_DIM)], w_sem.at[slot, n])
            for n, w in enumerate((wq_ref, wk_ref, wv_ref))
        ]

    def remote(p):
        head = head_at(p)
        target = owner_of(head, group, heads)
        slot = head - first_head(target, group, heads)
        copy = pltpu.make_async_remote_copy(
            src_ref=stage.at[p],
            dst_ref=land.at[slot, me],
            send_sem=send_sem.at[p],
            recv_sem=recv_sem.at[slot, me],
            device_id={"sp": target},
            device_id_type=MESH,
        )
        local = pltpu.make_async_copy(stage.at[p], land.at[slot, me], own_sem.at[slot])
        return target, copy, local

    def send(p):
        target, copy, local = remote(p)

        @pl.when(target != me)
        def _():
            copy.start()

        @pl.when(target == me)
        def _():
            local.start()

    for p in range(depth - 1):
        for c in weight_copies(p):
            c.start()
    greet_group(group, me)

    def project(p, carry):
        @pl.when(p + depth - 1 < heads)
        def _():
            for c in weight_copies(p + depth - 1):
                c.start()

        for c in weight_copies(p):
            c.wait()
        lin = jnp.dot(a_ref[...], wbuf[p % depth], preferred_element_type=jnp.float32)
        lin = lin + jnp.concatenate([vec_ref[:, pl.ds(pl.multiple_of(at + head_at(p) * HEAD_DIM, HEAD_DIM), HEAD_DIM)] for at in bias_at], axis=1)

        @pl.when(p > 0)
        def _():
            send(p - 1)

        cos_t, sin_t = cos_ref[...], sin_ref[...]
        for n in range(3):
            part = lin[:, n * HEAD_DIM:(n + 1) * HEAD_DIM]
            if n < 2:
                part = part * cos_t + pltpu.roll(part, HEAD_DIM // 2, 1) * sin_t
            stage[p, n] = part.astype(jnp.bfloat16)
        return carry

    lax.fori_loop(0, heads, project, 0)

    def clear(c, carry):
        for slot in range(slots):
            top_ref[slot, c] = jnp.full((rows, HEAD_DIM), -1e30, jnp.float32)
            sum_ref[slot, c] = jnp.zeros((rows, HEAD_DIM), jnp.float32)
            acc_ref[slot, c] = jnp.zeros((rows, HEAD_DIM), jnp.float32)
        return carry

    send(heads - 1)
    lax.fori_loop(0, chips, clear, 0)
    scale = HEAD_DIM ** -0.5 * 1.4426950408889634

    def chip_at(t):
        step = (t + 1) // 2
        return (my_chip + (2 * (t % 2) - 1) * step + chips) % chips

    def block(slot, part, chip):
        return land[slot, pl.ds(2 * chip, 2), part].reshape(rows, HEAD_DIM)

    def attend(slot, q_chip, k_chip, causal):
        scores = lax.dot_general(block(slot, 0, q_chip), block(slot, 1, k_chip), (((1,), (1,)), ((), ())), preferred_element_type=jnp.float32)
        q_pos = q_chip * rows + lax.broadcasted_iota(jnp.int32, (rows, 1), 0)
        q_low = jnp.zeros((rows, 1), jnp.int32)
        for d in range(1, cuts + 1):
            q_low = jnp.where(q_pos >= cu_ref[d], cu_ref[d], q_low)
        k_pos = k_chip * rows + lax.broadcasted_iota(jnp.int32, (1, rows), 1)
        seen = k_pos >= q_low
        if causal:
            seen = seen & (k_pos <= q_pos)
        scores = jnp.where(seen, scores, -1e30)
        top = top_ref[slot, q_chip]
        new_top = jnp.maximum(top, jnp.max(scores, axis=1, keepdims=True))
        decay = jnp.exp2((top - new_top) * scale)
        total = sum_ref[slot, q_chip] * decay
        parts = []
        for n in range(rows // HEAD_DIM):
            probs = jnp.exp2((scores[:, n * HEAD_DIM:(n + 1) * HEAD_DIM] - new_top) * scale)
            total = total + probs
            parts.append(probs.astype(jnp.bfloat16))
        mixed = jnp.dot(jnp.concatenate(parts, axis=1), block(slot, 2, k_chip), preferred_element_type=jnp.float32)
        top_ref[slot, q_chip] = new_top
        sum_ref[slot, q_chip] = total
        acc_ref[slot, q_chip] = acc_ref[slot, q_chip] * decay + mixed

    def for_slots(action):
        lax.fori_loop(0, count, lambda slot, carry: (action(slot), carry)[1], 0)

    def wait_chip(chip):
        def one(slot):
            for core in range(2):
                dev = 2 * chip + core
                landed = land.at[slot, dev]

                @pl.when(dev != me)
                def _():
                    pltpu.make_async_copy(landed, landed, recv_sem.at[slot, dev]).wait()

                @pl.when(dev == me)
                def _():
                    pltpu.make_async_copy(landed, landed, own_sem.at[slot]).wait()

        for_slots(one)

    def pair(t, u):
        here, there = chip_at(t), chip_at(u)
        later = (here - there + chips) // chips
        q_chip = here * later + there * (1 - later)
        k_chip = there * later + here * (1 - later)
        for_slots(lambda slot: attend(slot, q_chip, k_chip, False))

    def o_copy(slot, dev):
        return pltpu.make_async_remote_copy(
            src_ref=o_ref.at[slot, dev],
            dst_ref=attn_ref.at[mine + slot],
            send_sem=o_send.at[slot, dev],
            recv_sem=o_recv.at[mine + slot],
            device_id={"sp": dev},
            device_id_type=MESH,
        )

    def o_local(slot):
        return pltpu.make_async_copy(o_ref.at[slot, me], attn_ref.at[mine + slot], o_own.at[slot])

    def finish(chip):
        def divide(slot):
            total = jnp.sum(sum_ref[slot, chip], axis=1, keepdims=True)
            out = (acc_ref[slot, chip] / total).astype(jnp.bfloat16)
            o_ref[slot, pl.ds(2 * chip, 2)] = out.reshape(2, tokens, HEAD_DIM)

        def give(slot):
            for core in range(2):
                dev = 2 * chip + core

                @pl.when(dev != me)
                def _():
                    o_copy(slot, dev).start()

                @pl.when(dev == me)
                def _():
                    o_local(slot).start()

        for_slots(divide)
        for_slots(give)

    def arrival(t, carry):
        chip = chip_at(t)
        wait_chip(chip)
        for_slots(lambda slot: attend(slot, chip, chip, True))
        lax.fori_loop(0, t, lambda u, c: (pair(t, u), c)[1], 0)
        return carry

    last = chips - 1
    far = chip_at(last)
    lax.fori_loop(0, last, arrival, 0)

    def early(u, carry):
        @pl.when(chip_at(u) < far)
        def _():
            finish(chip_at(u))

        return carry

    lax.fori_loop(0, last, early, 0)
    wait_chip(far)
    for_slots(lambda slot: attend(slot, far, far, True))

    def late(u, carry):
        pair(last, u)

        @pl.when(chip_at(u) > far)
        def _():
            finish(chip_at(u))

        return carry

    lax.fori_loop(0, last, late, 0)
    finish(far)

    def drain(p, carry):
        target, copy, _ = remote(p)

        @pl.when(target != me)
        def _():
            copy.wait_send()

        return carry

    lax.fori_loop(0, heads, drain, 0)

    def drain_out(slot):
        def one(dev, carry):
            @pl.when(dev != me)
            def _():
                o_copy(slot, dev).wait_send()

            return carry

        lax.fori_loop(0, group, one, 0)
        o_local(slot).wait()

    for_slots(drain_out)

    def landed_out(head, carry):
        @pl.when(owner_of(head, group, heads) != me)
        def _():
            back = attn_ref.at[head]
            pltpu.make_async_copy(back, back, o_recv.at[head]).wait()

        return carry

    lax.fori_loop(0, heads, landed_out, 0)


def mixer(group, heads, cu_doc, normed, cos_t, sin_t, vectors, bias_at, w_q, w_k, w_v):
    tokens, width = normed.shape
    slots = -(-heads // group)
    chips = group // 2
    vmem = pl.BlockSpec(memory_space=pltpu.VMEM)
    smem = pl.BlockSpec(memory_space=pltpu.SMEM)
    hbm = pl.BlockSpec(memory_space=pl.ANY)
    state = pltpu.VMEM((slots, chips, 2 * tokens, HEAD_DIM), jnp.float32)
    return pl.pallas_call(
        functools.partial(mixer_kernel, group, heads, cu_doc.shape[0] - 2, bias_at),
        out_shape=jax.ShapeDtypeStruct((heads, tokens, HEAD_DIM), jnp.bfloat16),
        in_specs=[smem, vmem, vmem, vmem, vmem, hbm, hbm, hbm],
        out_specs=hbm,
        scratch_shapes=[
            pltpu.VMEM((3, width, 3 * HEAD_DIM), jnp.bfloat16),
            pltpu.VMEM((heads, 3, tokens, HEAD_DIM), jnp.bfloat16),
            pltpu.VMEM((slots, group, 3, tokens, HEAD_DIM), jnp.bfloat16),
            state,
            state,
            state,
            pltpu.VMEM((slots, group, tokens, HEAD_DIM), jnp.bfloat16),
            pltpu.SemaphoreType.DMA((3, 3)),
            pltpu.SemaphoreType.DMA((heads,)),
            pltpu.SemaphoreType.DMA((slots, group)),
            pltpu.SemaphoreType.DMA((slots,)),
            pltpu.SemaphoreType.DMA((slots, group)),
            pltpu.SemaphoreType.DMA((heads,)),
            pltpu.SemaphoreType.DMA((slots,)),
        ],
        compiler_params=pltpu.CompilerParams(collective_id=0, has_side_effects=True, vmem_limit_bytes=MIXER_VMEM),
        cost_estimate=pl.CostEstimate(flops=2 * tokens * width * 3 * heads * HEAD_DIM, bytes_accessed=3 * width * heads * HEAD_DIM * 2, transcendentals=0),
        name="mixer",
    )(cu_doc, normed, cos_t, sin_t, vectors, w_q, w_k, w_v)


def merge_place_kernel(group, patch_ref, vec_ref, slots_ref, embeds_ref, w1_ref, w2_ref, h_ref, a_ref, z, scaled, wbuf, inner, wide, rows, slots, total, hits, w_sem, z_send, z_recv, in_send, in_recv, slot_send, slot_recv, ring_send, ring_recv, pair_send, pair_recv):
    me = lax.axis_index("sp")
    core = me % 2
    chip = me // 2
    chips = group // 2
    other = me + 1 - 2 * core
    ahead = (me + 2 - 4 * core + group) % group
    depth = wbuf.shape[0]
    part, span = rows.shape[-1], wbuf.shape[2]
    merged_dev, vit = slots_ref.shape[1], patch_ref.shape[1]
    merge_dim, width = w2_ref.shape
    half_in, half_out = merge_dim // (2 * span), width // (2 * part)
    spans = [min(span, width // 2 - at) for at in range(0, width // 2, span)]
    count = half_in + len(spans)
    after = [0]
    for size in (vit, vit, merge_dim, width, width):
        after.append(after[-1] + size)

    def vector(n):
        return vec_ref[:, after[n]:after[n + 1]]

    def bias(n, at, size):
        return vec_ref[:, pl.ds(pl.multiple_of(after[n] + at, HEAD_DIM), size)]

    def weight_copy(j):
        slot = j % depth
        if j < half_in:
            w_ref, at, size = w1_ref, core * (merge_dim // 2) + j * span, span
        else:
            w_ref, at, size = w2_ref, core * (width // 2) + (j - half_in) * span, spans[j - half_in]
        return pltpu.make_async_copy(w_ref.at[:, pl.ds(pl.multiple_of(at, HEAD_DIM), size)], wbuf.at[slot, :, pl.ds(0, size)], w_sem.at[slot])

    for j in range(depth - 1):
        weight_copy(j).start()
    widened = patch_ref[...].astype(jnp.float32)
    centered = widened - jnp.mean(widened, axis=-1, keepdims=True)
    spread = jnp.mean(centered * centered, axis=-1, keepdims=True)
    normed = centered * lax.rsqrt(spread + NORM_EPS) * vector(0) + vector(1)
    for c in range(vit // HEAD_DIM):
        scaled[c] = normed[:, c * HEAD_DIM:(c + 1) * HEAD_DIM]
    merge = merge_dim // vit
    for n in range(merge):
        for c in range(vit // HEAD_DIM):
            lanes = n * vit + c * HEAD_DIM
            z[core, :, lanes:lanes + HEAD_DIM] = scaled[c, pl.ds(n, merged_dev, stride=merge), :].astype(jnp.bfloat16)
    total[...] = jnp.zeros_like(total)
    hits[...] = jnp.zeros_like(hits)
    slots[me] = slots_ref[...]
    greet_group(group, me)

    def to_other(src, dst, send_sem, recv_sem):
        return pltpu.make_async_remote_copy(src_ref=src, dst_ref=dst, send_sem=send_sem, recv_sem=recv_sem, device_id={"sp": other}, device_id_type=MESH)

    def arrive(ref, sem):
        pltpu.make_async_copy(ref, ref, sem).wait()

    def slot_copy(k):
        return pltpu.make_async_remote_copy(
            src_ref=slots_ref, dst_ref=slots.at[me], send_sem=slot_send.at[k], recv_sem=slot_recv.at[me],
            device_id={"sp": lax.rem(me + k, group)}, device_id_type=MESH,
        )

    z_copy = to_other(z.at[core], z.at[core], z_send, z_recv)
    z_copy.start()
    for k in range(1, group):
        slot_copy(k).start()
    arrive(z.at[1 - core], z_recv)

    def inner_copy(j):
        mine = inner.at[core * half_in + j]
        return to_other(mine, mine, in_send.at[j], in_recv.at[j])

    def origin(lane, step):
        return (chip - (1 - 2 * lane) * step + chips) % chips

    def ring_copy(step, piece):
        held = rows.at[core, origin(core, step), piece]
        return pltpu.make_async_remote_copy(
            src_ref=held, dst_ref=held, send_sem=ring_send.at[step, piece], recv_sem=ring_recv.at[step, piece],
            device_id={"sp": ahead}, device_id_type=MESH,
        )

    def pair_copy(step, piece):
        held = rows.at[core, origin(core, step), piece]
        return to_other(held, held, pair_send.at[step, piece], pair_recv.at[step, piece])

    for j in range(half_in):
        weight_copy(j + depth - 1).start()
        weight_copy(j).wait()
        lin = jnp.dot(z[...].reshape(2 * merged_dev, merge_dim), wbuf[j % depth], preferred_element_type=jnp.float32)
        lin = lin + bias(2, (core * half_in + j) * span, span)
        inner[core * half_in + j] = (lin * (0.5 * (1.0 + lax.erf(lin * 0.7071067811865476)))).astype(jnp.bfloat16)
        if j > 0:
            inner_copy(j - 1).start()
    inner_copy(half_in - 1).start()
    for j in range(half_in):
        arrive(inner.at[(1 - core) * half_in + j], in_recv.at[j])
    for j in range(2 * half_in):
        wide[:, j * span:(j + 1) * span] = inner[j]
    made, pending = 0, []
    for j in range(half_in, count):
        size = spans[j - half_in]
        if j + depth - 1 < count:
            weight_copy(j + depth - 1).start()
        weight_copy(j).wait()
        lin = jnp.dot(wide[...], wbuf[j % depth, :, :size], preferred_element_type=jnp.float32)
        lin = (lin + bias(3, core * (width // 2) + (j - half_in) * span, size)).astype(jnp.bfloat16)
        fresh = range(made, made + size // part)
        for piece in fresh:
            rows[core, chip, piece] = lin[:, (piece - made) * part:(piece - made + 1) * part]
        for piece in pending:
            ring_copy(0, piece).start()
            pair_copy(0, piece).start()
        made, pending = made + size // part, fresh
    tokens = embeds_ref.shape[0]
    wanted = me * tokens + lax.broadcasted_iota(jnp.int32, (tokens, 1), 0)
    for k in range(1, group):
        dev = lax.rem(me + k, group)
        arrive(slots.at[dev], slot_recv.at[dev])
    for piece in pending:
        ring_copy(0, piece).start()
        pair_copy(0, piece).start()

    def choose(block):
        return jnp.concatenate([jnp.where(slots[2 * block + n] == wanted, 1.0, 0.0) for n in range(2)], axis=1)

    def place(lane, block, piece, pick):
        total[lane * half_out + piece] += jnp.dot(pick, rows[lane, block, piece], preferred_element_type=jnp.float32)

    def hop(step, carry):
        mine, theirs = origin(core, step - 1), origin(1 - core, step - 1)
        pick, pick_theirs = choose(mine), choose(theirs).astype(jnp.bfloat16)
        hits[...] += pick
        pick = pick.astype(jnp.bfloat16)
        for piece in range(half_out):

            @pl.when(step < chips)
            def _():
                arrive(rows.at[core, origin(core, step), piece], ring_recv.at[step - 1, piece])

                @pl.when(step < chips - 1)
                def _():
                    ring_copy(step, piece).start()

                pair_copy(step, piece).start()

            place(core, mine, piece, pick)
            arrive(rows.at[1 - core, theirs, piece], pair_recv.at[step - 1, piece])
            place(1 - core, theirs, piece, pick_theirs)
        return carry

    lax.fori_loop(1, chips + 1, hop, 0)
    found = jnp.max(hits[...], axis=1, keepdims=True) > 0.0
    for n in range(2 * half_out):
        cols = slice(n * part, (n + 1) * part)
        h_ref[:, cols] = jnp.where(found, total[n].astype(jnp.bfloat16), embeds_ref[:, cols])
    a_ref[...] = rms_norm(h_ref[...], vector(4))
    z_copy.wait_send()
    for k in range(1, group):
        slot_copy(k).wait_send()
    for j in range(half_in):
        inner_copy(j).wait_send()

    def drain(step, carry):
        for piece in range(half_out):
            @pl.when(step < chips - 1)
            def _():
                ring_copy(step, piece).wait_send()

            pair_copy(step, piece).wait_send()
        return carry

    lax.fori_loop(0, chips, drain, 0)


def merge_place(group, patches, vectors, w_one, w_two, dest_slot, embeds):
    merged_dev = dest_slot.shape[0]
    merge_dim, width = w_two.shape
    tokens = embeds.shape[0]
    part = 2 * HEAD_DIM
    chips = group // 2
    span = 2 * part
    n_in, n_out = merge_dim // span, width // part
    vmem = pl.BlockSpec(memory_space=pltpu.VMEM)
    hbm = pl.BlockSpec(memory_space=pl.ANY)
    out = jax.ShapeDtypeStruct((tokens, width), jnp.bfloat16)
    ring = pltpu.SemaphoreType.DMA((chips, n_out // 2))
    return pl.pallas_call(
        functools.partial(merge_place_kernel, group),
        out_shape=(out, out),
        in_specs=[vmem] * 4 + [hbm, hbm],
        out_specs=(vmem, vmem),
        scratch_shapes=[
            pltpu.VMEM((2, merged_dev, merge_dim), jnp.bfloat16),
            pltpu.VMEM((patches.shape[1] // HEAD_DIM, patches.shape[0], HEAD_DIM), jnp.float32),
            pltpu.VMEM((3, merge_dim, span), jnp.bfloat16),
            pltpu.VMEM((n_in, 2 * merged_dev, span), jnp.bfloat16),
            pltpu.VMEM((2 * merged_dev, merge_dim), jnp.bfloat16),
            pltpu.VMEM((2, chips, n_out // 2, 2 * merged_dev, part), jnp.bfloat16),
            pltpu.VMEM((group, 1, merged_dev), jnp.int32),
            pltpu.VMEM((n_out, tokens, part), jnp.float32),
            pltpu.VMEM((tokens, 2 * merged_dev), jnp.float32),
            pltpu.SemaphoreType.DMA((3,)),
            pltpu.SemaphoreType.DMA,
            pltpu.SemaphoreType.DMA,
            pltpu.SemaphoreType.DMA((n_in // 2,)),
            pltpu.SemaphoreType.DMA((n_in // 2,)),
            pltpu.SemaphoreType.DMA((group,)),
            pltpu.SemaphoreType.DMA((group,)),
            ring,
            ring,
            ring,
            ring,
        ],
        compiler_params=pltpu.CompilerParams(collective_id=2, has_side_effects=True, vmem_limit_bytes=VMEM_LIMIT),
        cost_estimate=pl.CostEstimate(flops=2 * merged_dev * merge_dim * (merge_dim + width), bytes_accessed=merge_dim * (merge_dim + width), transcendentals=0),
        name="merge_place",
    )(
        patches, vectors,
        dest_slot.reshape(1, merged_dev), embeds, w_one, w_two,
    )


def mlp_kernel(o_cols, chunk, gain_at, attn_ref, h_ref, vec_ref, wo_ref, wg_ref, wu_ref, wd_ref, out_ref, attn, h_one, normed, total, wo, wg, wu, wd, o_sem, f_sem):
    heads, _, dim = attn_ref.shape
    width = h_ref.shape[1]
    o_steps, steps = width // o_cols, wg_ref.shape[1] // chunk

    def o_copy(i):
        return pltpu.make_async_copy(wo_ref.at[:, pl.ds(i * o_cols, o_cols)], wo.at[i % 2], o_sem.at[i % 2])

    def f_copies(i):
        b = i % 2
        cols = pl.ds(pl.multiple_of(i * chunk, 128), chunk)
        return [
            pltpu.make_async_copy(wg_ref.at[:, cols], wg.at[b], f_sem.at[b, 0]),
            pltpu.make_async_copy(wu_ref.at[:, cols], wu.at[b], f_sem.at[b, 1]),
            pltpu.make_async_copy(wd_ref.at[cols, :], wd.at[b], f_sem.at[b, 2]),
        ]

    o_copy(0).start()
    o_copy(1).start()
    for h in range(heads):
        attn[:, h * dim:(h + 1) * dim] = attn_ref[h]
    for i in range(o_steps):
        o_copy(i).wait()
        cols = slice(i * o_cols, (i + 1) * o_cols)
        part = jnp.dot(attn[...], wo[i % 2], preferred_element_type=jnp.float32)
        h_one[:, cols] = (h_ref[:, cols].astype(jnp.float32) + part).astype(jnp.bfloat16)
        if i + 2 < o_steps:
            o_copy(i + 2).start()
        if i == o_steps - 3:
            for c in f_copies(0):
                c.start()
    normed[...] = rms_norm(h_one[...], vec_ref[:, gain_at:gain_at + width])
    total[...] = h_one[...].astype(jnp.float32)

    def step(i, carry):
        b = i % 2

        @pl.when(i + 1 < steps)
        def _():
            for c in f_copies(i + 1):
                c.start()

        gate_copy, up_copy, down_copy = f_copies(i)
        gate_copy.wait()
        up_copy.wait()
        gate_pre = jnp.dot(normed[...], wg[b], preferred_element_type=jnp.float32)
        up_pre = jnp.dot(normed[...], wu[b], preferred_element_type=jnp.float32)
        activated = (jax.nn.silu(gate_pre) * up_pre).astype(jnp.bfloat16)
        down_copy.wait()
        total[...] += jnp.dot(activated, wd[b], preferred_element_type=jnp.float32)
        return carry

    lax.fori_loop(0, steps, step, 0)
    out_ref[...] = total[...].astype(jnp.bfloat16)


def mlp(attn, h_zero, vectors, gain_at, w_o, w_gate, w_up, w_down):
    heads, tokens, dim = attn.shape
    width, ffn = w_gate.shape
    o_cols = width // 5
    chunk = ffn // 9
    vmem = pl.BlockSpec(memory_space=pltpu.VMEM)
    hbm = pl.BlockSpec(memory_space=pl.ANY)
    return pl.pallas_call(
        functools.partial(mlp_kernel, o_cols, chunk, gain_at),
        out_shape=jax.ShapeDtypeStruct((tokens, width), jnp.bfloat16),
        in_specs=[vmem, vmem, vmem, hbm, hbm, hbm, hbm],
        out_specs=vmem,
        scratch_shapes=[
            pltpu.VMEM((tokens, heads * dim), jnp.bfloat16),
            pltpu.VMEM((tokens, width), jnp.bfloat16),
            pltpu.VMEM((tokens, width), jnp.bfloat16),
            pltpu.VMEM((tokens, width), jnp.float32),
            pltpu.VMEM((2, heads * dim, o_cols), jnp.bfloat16),
            pltpu.VMEM((2, width, chunk), jnp.bfloat16),
            pltpu.VMEM((2, width, chunk), jnp.bfloat16),
            pltpu.VMEM((2, chunk, width), jnp.bfloat16),
            pltpu.SemaphoreType.DMA((2,)),
            pltpu.SemaphoreType.DMA((2, 3)),
        ],
        compiler_params=pltpu.CompilerParams(vmem_limit_bytes=MLP_VMEM),
        cost_estimate=pl.CostEstimate(flops=2 * tokens * width * (3 * ffn + width), bytes_accessed=2 * width * (3 * ffn + width), transcendentals=tokens * ffn),
        name="mlp",
    )(attn, h_zero, vectors, w_o, w_gate, w_up, w_down)


def solution(mesh):
    group = mesh.shape['sp']
    row_spec = P(('dp', 'sp'), None)

    def local_step(patches, embeds, dest_slot, rope_pos, cu_doc, ln_w, ln_b, w_one, b_one, w_two, b_two, norm_attn, w_q, b_q, w_k, b_k, w_v, b_v, w_o, norm_mlp, w_gate, w_up, w_down):
        heads = w_q.shape[1] // HEAD_DIM
        parts = (ln_w, ln_b, b_one, b_two, norm_attn, b_q, b_k, b_v, norm_mlp)
        starts = [sum(v.shape[0] for v in parts[:n]) for n in range(len(parts))]
        length = starts[-1] + parts[-1].shape[0]
        vectors = sum(jnp.pad(v.astype(jnp.float32), (at, length - at - v.shape[0])) for at, v in zip(starts, parts)).reshape(1, length)
        cos_t, sin_t = rope_tables(rope_pos)
        h_zero, normed_a = merge_place(group, patches, vectors, w_one, w_two, dest_slot, embeds)
        attn_out = mixer(group, heads, cu_doc, normed_a, cos_t, sin_t, vectors, tuple(starts[5:8]), w_q, w_k, w_v)
        return mlp(attn_out, h_zero, vectors, starts[8], w_o, w_gate, w_up, w_down)

    in_specs = (row_spec, row_spec, P(('dp', 'sp')), P(None, ('dp', 'sp')), P('dp')) + (P(),) * 18
    return jax.shard_map(local_step, mesh=mesh, in_specs=in_specs, out_specs=row_spec, check_vma=False)
```
